32 devices in a mesh: row: 8 (over z, y), col: 4 (over x, core).
Axes of the slice: x: 2, y: 2, z: 4, core: 2. Of those that a mesh axis runs over, the one named last changes fastest.
Arguments:
- v_panels: float32 [4096, 4096], P('row', 'col')
- t_factors: float32 [128, 32, 32], P('col')
- z_vecs: float32 [4096, 4096], P(None, ('row', 'col'))
Outputs:
- output: float32 [4096, 4096], P(None, ('row', 'col'))
All inputs are finite; a program needn't handle non-finite values.
Results may differ from the reference program's by a relative error of at most 0.001.
Values sent between devices are 32-bit elements.
A program may use at most 1 GiB of HBM per device.

```python
import jax
import jax.numpy as jnp
from jax import lax

N = 4096
BLOCK = 32
K_DEV = 128
ROW_DEV = 8
COL_DEV = 4

NPANEL = N // BLOCK
M_LOC = NPANEL // COL_DEV
K_COLS = K_DEV * ROW_DEV * COL_DEV


def build_inputs(raw_vals, z_vecs):
    row_nat = jnp.arange(N)[:, None, None]
    diag_row = (jnp.arange(NPANEL) * BLOCK)[None, :, None] + jnp.arange(BLOCK)[None, None, :]
    v_nat = jnp.where(row_nat > diag_row, raw_vals, jnp.where(row_nat == diag_row, 1.0, 0.0)).astype(raw_vals.dtype)
    gram = jnp.einsum("nmb,nmc->mbc", v_nat, v_nat, precision=lax.Precision.HIGHEST)
    half_diag = 0.5 * jnp.diagonal(gram, axis1=1, axis2=2)
    t_inverse = jnp.triu(gram, 1) + jnp.eye(BLOCK, dtype=raw_vals.dtype) * half_diag[:, None, :]
    t_nat = jnp.triu(jnp.linalg.inv(t_inverse))
    v_cols = v_nat.reshape(N, M_LOC, COL_DEV, BLOCK).transpose(0, 2, 1, 3).reshape(N, N)
    v_store = v_cols.reshape(NPANEL // ROW_DEV, ROW_DEV, BLOCK, N).transpose(1, 0, 2, 3).reshape(N, N)
    t_store = t_nat.reshape(M_LOC, COL_DEV, BLOCK, BLOCK).transpose(1, 0, 2, 3).reshape(NPANEL, BLOCK, BLOCK)
    return {"v_panels": v_store, "t_factors": t_store, "z_vecs": z_vecs}


def setup_inputs(seed: int = 0) -> dict:
    base_key = jax.random.key(seed)
    key_v, key_z = jax.random.split(base_key)
    raw_vals = jax.random.normal(key_v, (N, NPANEL, BLOCK), jnp.float32)
    z_vecs = jax.random.normal(key_z, (N, K_COLS), jnp.float32)
    return build_inputs(raw_vals, z_vecs)


def reference(v_panels, t_factors, z_vecs):
    def apply_panel(x_cur, panel_idx):
        store_slot = (panel_idx % COL_DEV) * M_LOC + panel_idx // COL_DEV
        v_blk = lax.dynamic_slice_in_dim(v_panels, store_slot * BLOCK, BLOCK, axis=1)
        t_blk = lax.dynamic_index_in_dim(t_factors, store_slot, axis=0, keepdims=False)
        w_blk = jnp.dot(v_blk.T, x_cur, precision=lax.Precision.HIGHEST, preferred_element_type=jnp.float32)
        y_blk = jnp.dot(t_blk, w_blk, precision=lax.Precision.HIGHEST, preferred_element_type=jnp.float32)
        x_new = x_cur - jnp.dot(v_blk, y_blk, precision=lax.Precision.HIGHEST, preferred_element_type=jnp.float32)
        return x_new, None

    x_out, _ = lax.scan(apply_panel, z_vecs, jnp.arange(NPANEL - 1, -1, -1))
    return x_out
```

```python
import functools
import jax
import jax.numpy as jnp
from jax import lax
from jax.experimental import pallas as pl
from jax.experimental.pallas import tpu as pltpu
from jax.sharding import PartitionSpec as P

F32 = jnp.float32
BF16 = jnp.bfloat16
HI = lax.Precision.HIGHEST
GROUPS = ((1, 4), (5, 6), (7, 8), (9, 10), (11, 12), (13, 14), (15, 15), (16, 16))


def split3(v):
    h = v.astype(BF16)
    r = v - h.astype(F32)
    m = r.astype(BF16)
    l = (r - m.astype(F32)).astype(BF16)
    return h, m, l


def bdot(a, b):
    return jnp.dot(a, b, preferred_element_type=F32)


def fdot(a, b):
    return jnp.dot(a, b, precision=HI, preferred_element_type=F32)


def group_kernel(n_lo, n_hi, ag_ref, t_ref, x_in, x_ref, vin, tin, vh_s, vm_s, vl_s, gp_s, a_s, q_s, sem, tsem):
    def off(n):
        return pl.multiple_of(8 * (n * (n - 1) - n_lo * (n_lo - 1)), 16)

    def fetch(n, slot):
        base = off(n)

        def one(k, _):
            pltpu.make_async_copy(ag_ref.at[:, pl.ds(base + 16 * k, 16), :], vin.at[slot, k], sem.at[slot]).start()
            return 0

        lax.fori_loop(0, n, one, 0)
        pltpu.make_async_copy(t_ref.at[:, pl.ds(pl.multiple_of(64 * (16 - n), 64), 64), :], tin.at[slot], tsem.at[slot]).start()

    def arrive(n, slot):
        def one(k, _):
            pltpu.make_async_copy(ag_ref.at[:, pl.ds(0, 16), :], vin.at[slot, k], sem.at[slot]).wait()
            return 0

        lax.fori_loop(0, n, one, 0)
        pltpu.make_async_copy(t_ref.at[:, pl.ds(0, 64), :], tin.at[slot], tsem.at[slot]).wait()

    fetch(jnp.int32(n_lo), jnp.int32(0))
    x_ref[...] = x_in[...]

    ia = lax.broadcasted_iota(jnp.int32, (256, 256), 0) // 32
    ib = lax.broadcasted_iota(jnp.int32, (256, 256), 1) // 32

    def superblock(n, _):
        slot = lax.rem(n - n_lo, 2)
        arrive(n, slot)

        @pl.when(n < n_hi)
        def _():
            fetch(n + 1, 1 - slot)

        b = 16 - n
        gp_s[...] = jnp.zeros_like(gp_s)
        a_s[...] = jnp.zeros_like(a_s)
        q_s[...] = jnp.zeros_like(q_s)
        low = lax.broadcasted_iota(jnp.int32, (8, 16, 128), 2) < 64

        def gram(k, _):
            blk = vin[slot, k].reshape(8, 4, 16, 128)
            p = [blk[:, c] for c in range(4)]
            s = [pltpu.roll(q.reshape(128, 128), 64, 1).reshape(8, 16, 128) for q in p]
            top = jnp.concatenate([jnp.where(low, p[0], s[1]), jnp.where(low, p[2], s[3])], axis=2)
            bot = jnp.concatenate([jnp.where(low, s[0], p[1]), jnp.where(low, s[2], p[3])], axis=2)
            v = jnp.concatenate([top, bot], axis=1).reshape(256, 256)
            vh, vm, vl = split3(v)
            rows = pl.ds(pl.multiple_of(k * 256, 256), 256)
            vh_s[rows, :] = vh
            vm_s[rows, :] = vm
            vl_s[rows, :] = vl
            th, tm, tl = split3(v.T)
            x = x_ref[pl.ds(pl.multiple_of((b + k) * 256, 256), 256), :]
            xh, xm, xl = split3(x)
            x2 = jnp.concatenate([xh, xm], axis=1)
            gp_s[...] += bdot(
                jnp.concatenate([th, tm], axis=1),
                jnp.concatenate([jnp.concatenate([vh, x2], axis=1), jnp.concatenate([vm, x2], axis=1)], axis=0),
            )
            a_s[...] += bdot(jnp.concatenate([th, th], axis=1), jnp.concatenate([vm, vl], axis=0))
            q_s[...] += bdot(jnp.concatenate([tl, th], axis=1), jnp.concatenate([xh, xl], axis=0))
            return 0

        lax.fori_loop(0, n, gram, 0)

        a = a_s[...]
        g = gp_s[:, :256] + (a + a.T)
        w = (q_s[...] + gp_s[:, 384:]) + gp_s[:, 256:384]
        na = 4 * (ia % 2) + ia // 2
        nb = 4 * (ib % 2) + ib // 2
        t4 = tin[slot].reshape(256, 128)
        t = jnp.where(ia == ib, jnp.concatenate([t4, t4], axis=1), 0.0)
        for lev in (1, 2, 4):
            pick = (na // (2 * lev) == nb // (2 * lev)) & ((na // lev) % 2 == 0) & ((nb // lev) % 2 == 1)
            t = t - fdot(fdot(t, jnp.where(pick, g, 0.0)), t)
        yh, ym, yl = split3(fdot(t, w))
        y2 = jnp.concatenate([yh, ym], axis=1)
        y22 = jnp.concatenate([y2, y2], axis=0)
        yq = jnp.concatenate([yh, yl], axis=0)

        def update(k, _):
            rows = pl.ds(pl.multiple_of(k * 256, 256), 256)
            vh = vh_s[rows, :]
            z2 = bdot(jnp.concatenate([vh, vm_s[rows, :]], axis=1), y22)
            zq = bdot(jnp.concatenate([vl_s[rows, :], vh], axis=1), yq)
            xr = pl.ds(pl.multiple_of((b + k) * 256, 256), 256)
            x_ref[xr, :] = x_ref[xr, :] - ((zq + z2[:, 128:]) + z2[:, :128])
            return 0

        lax.fori_loop(0, n, update, 0)
        return 0

    lax.fori_loop(n_lo, n_hi + 1, superblock, 0)


def run_group(n_lo, n_hi, ag, t_all, x, interpret=False):
    return pl.pallas_call(
        functools.partial(group_kernel, n_lo, n_hi),
        out_shape=jax.ShapeDtypeStruct((4096, 128), F32),
        in_specs=[pl.BlockSpec(memory_space=pl.ANY), pl.BlockSpec(memory_space=pl.ANY), pl.BlockSpec(memory_space=pltpu.VMEM)],
        out_specs=pl.BlockSpec(memory_space=pltpu.VMEM),
        scratch_shapes=[
            pltpu.VMEM((2, 16, 32, 16, 128), F32),
            pltpu.VMEM((2, 4, 64, 128), F32),
            pltpu.VMEM((4096, 256), BF16),
            pltpu.VMEM((4096, 256), BF16),
            pltpu.VMEM((4096, 256), BF16),
            pltpu.VMEM((256, 512), F32),
            pltpu.VMEM((256, 256), F32),
            pltpu.VMEM((256, 128), F32),
            pltpu.SemaphoreType.DMA((2,)),
            pltpu.SemaphoreType.DMA((2,)),
        ],
        compiler_params=pltpu.CompilerParams(vmem_limit_bytes=48 * 1024 * 1024),
        cost_estimate=pl.CostEstimate(flops=sum(range(n_lo, n_hi + 1)) * 6 * 2 * 256 * 256 * 700, bytes_accessed=8 << 20, transcendentals=0),
        name=f"apply_{n_lo}_{n_hi}",
        interpret=interpret,
    )(ag, t_all, x)


def pack_piece(v_loc, n):
    b = 16 - n
    piece = v_loc[32 * b :, 64 * b : 64 * b + 64]
    return piece.reshape(n, 2, 16, 64).transpose(0, 2, 1, 3).reshape(16 * n, 128)


def solution(mesh):
    def local_apply(v_loc, t_loc, z_loc):
        t4 = jnp.tile(t_loc.reshape(1024, 32), (1, 4))
        t_all = lax.all_gather(t4, "col")
        gathered = []
        for n_lo, n_hi in GROUPS:
            piece = jnp.concatenate([pack_piece(v_loc, n) for n in range(n_lo, n_hi + 1)], axis=0)
            gathered.append(lax.all_gather(piece, ("row", "col")))
        x = z_loc.reshape(8, 16, 32, 128).transpose(1, 0, 2, 3).reshape(4096, 128)
        for (n_lo, n_hi), ag in zip(GROUPS, gathered):
            x = run_group(n_lo, n_hi, ag, t_all, x)
        return x.reshape(16, 8, 32, 128).transpose(1, 0, 2, 3).reshape(4096, 128)

    return jax.shard_map(
        local_apply,
        mesh=mesh,
        in_specs=(P("row", "col"), P("col", None, None), P(None, ("row", "col"))),
        out_specs=P(None, ("row", "col")),
        check_vma=False,
    )
```

```python
import functools
import jax
import jax.numpy as jnp
from jax import lax
from jax.experimental import pallas as pl
from jax.experimental.pallas import tpu as pltpu
from jax.sharding import PartitionSpec as P

F32 = jnp.float32
BF16 = jnp.bfloat16
HI = lax.Precision.HIGHEST
MESH = pl.DeviceIdType.MESH
UNITS = 36
Z_AHEAD = 6
D1 = 2
D2 = 2
LEAD = 0
LAG = D1 + D2


def split3(v):
    h = v.astype(BF16)
    r = v - h.astype(F32)
    m = r.astype(BF16)
    l = (r - m.astype(F32)).astype(BF16)
    return h, m, l


def bdot(a, b):
    return jnp.dot(a, b, preferred_element_type=F32)


def fdot(a, b):
    return jnp.dot(a, b, precision=HI, preferred_element_type=F32)


def loop(lo, hi, body):
    def step(i, carry):
        body(i)
        return carry

    lax.fori_loop(lo, hi, step, 0)


def fused_kernel(
    v_ref, t_ref, z_ref, o_ref, buf, tbuf, xbuf, vh_s, vm_s, vl_s, gp_s, a_s, q_s,
    in_sem, send_sem, z_sem, x1_sem, y1_sem, x2_sem, y2_sem, p_sem, t_sem,
):
    row, col = lax.axis_index("row"), lax.axis_index("col")
    z, y = row // 2, lax.rem(row, 2)
    x, c = col // 2, lax.rem(col, 2)
    x_dev = (row, (1 - x) * 2 + c)
    y_dev = (z * 2 + 1 - y, col)
    p_dev = (row, x * 2 + 1 - c)
    z_devs = [(lax.rem(z + k, 4) * 2 + y, col) for k in (1, 2, 3)]

    def unit(q):
        return pl.ds(pl.multiple_of(64 * q, 64), 64)

    def remote(view, recv, dev, kind):
        return pltpu.make_async_remote_copy(
            src_ref=view, dst_ref=view, send_sem=send_sem.at[kind], recv_sem=recv, device_id=dev, device_id_type=MESH
        )

    def z_copy(q, k):
        return remote(buf.at[c, x, y, z, unit(q)], z_sem.at[q], z_devs[k], 0)

    def x1_copy(q):
        return remote(buf.at[c, x, y, :, unit(q)], x1_sem.at[q], x_dev, 1)

    def y1_copy(q):
        return remote(buf.at[c, x, y, :, unit(q)], y1_sem.at[q], y_dev, 2)

    def y2_copy(q):
        return remote(buf.at[c, 1 - x, y, 0:2, unit(q)], y2_sem.at[q], y_dev, 3)

    def x2_copy(q):
        return remote(buf.at[c, x, 1 - y, 2:4, unit(q)], x2_sem.at[q], x_dev, 4)

    def p_copy(q, xx, yy):
        return remote(buf.at[c, xx, yy, :, unit(q)], p_sem.at[q], p_dev, 5)

    def z_land(q):
        return remote(buf.at[c, x, y, 0:3, unit(q)], z_sem.at[q], x_dev, 0)

    def x1_land(q):
        return remote(buf.at[c, 1 - x, y, :, unit(q)], x1_sem.at[q], x_dev, 1)

    def y1_land(q):
        return remote(buf.at[c, x, 1 - y, :, unit(q)], y1_sem.at[q], y_dev, 2)

    def y2_land(q):
        return remote(buf.at[c, 1 - x, 1 - y, 0:2, unit(q)], y2_sem.at[q], y_dev, 3)

    def x2_land(q):
        return remote(buf.at[c, 1 - x, 1 - y, 2:4, unit(q)], x2_sem.at[q], x_dev, 4)

    def p_land(q):
        return remote(buf.at[1 - c, :, :, :, unit(q)], p_sem.at[q], p_dev, 5)

    def z_send(q):
        for k in range(3):
            z_copy(q, k).start()

    def comm(q):
        @pl.when(q + Z_AHEAD < UNITS)
        def _():
            z_send(q + Z_AHEAD)

        @pl.when(q < UNITS)
        def _():
            z_land(q).wait_recv()
            x1_copy(q).start()
            y1_copy(q).start()
            p_copy(q, x, y).start()

        q1 = q - D1

        @pl.when((q1 >= 0) & (q1 < UNITS))
        def _():
            x1_land(q1).wait_recv()
            y2_copy(q1).start()
            y1_land(q1).wait_recv()
            x2_copy(q1).start()
            p_copy(q1, 1 - x, y).start()
            p_copy(q1, x, 1 - y).start()

        q2 = q - LAG

        @pl.when((q2 >= 0) & (q2 < UNITS))
        def _():
            y2_land(q2).wait_recv()
            x2_land(q2).wait_recv()
            p_copy(q2, 1 - x, 1 - y).start()

    def first_unit(n):
        return n * (n - 1) // 2

    def v_in(n, j):
        src = v_ref.at[pl.ds(pl.multiple_of(64 * (8 - n + j), 64), 64), pl.ds(pl.multiple_of(128 * (8 - n), 128), 128)]
        return pltpu.make_async_copy(src, buf.at[c, x, y, z, unit(first_unit(n) + j)], in_sem.at[0])

    def z_in(r):
        return pltpu.make_async_copy(z_ref.at[r], xbuf.at[:, lax.rem(r, 2), r // 2], in_sem.at[1])

    t_in = pltpu.make_async_copy(t_ref, tbuf.at[c, x], in_sem.at[2])
    loop(1, 9, lambda n: loop(0, n, lambda j: v_in(n, j).start()))
    t_in.start()
    loop(0, 8, lambda r: z_in(r).start())

    barrier = pltpu.get_barrier_semaphore()
    for dev in [x_dev, y_dev, p_dev] + z_devs:
        pl.semaphore_signal(barrier, inc=1, device_id=dev, device_id_type=MESH)
    own = buf.at[c, x, y, z]
    pltpu.make_async_copy(own, own, in_sem.at[0]).wait()
    pl.semaphore_wait(barrier, 6)

    loop(0, Z_AHEAD, z_send)
    t_in.wait()
    t_x = remote(tbuf.at[c, x], t_sem.at[0], x_dev, 6)
    t_p = [remote(tbuf.at[c, x], t_sem.at[1], p_dev, 7), remote(tbuf.at[c, 1 - x], t_sem.at[2], p_dev, 8)]
    t_x.start()
    t_p[0].start()
    loop(0, 1 + LAG + LEAD, comm)
    remote(tbuf.at[c, 1 - x], t_sem.at[0], x_dev, 6).wait_recv()
    t_p[1].start()
    pltpu.make_async_copy(xbuf, xbuf, in_sem.at[1]).wait()
    remote(tbuf.at[1 - c, x], t_sem.at[1], p_dev, 7).wait_recv()
    remote(tbuf.at[1 - c, 1 - x], t_sem.at[2], p_dev, 8).wait_recv()

    ia = lax.broadcasted_iota(jnp.int32, (256, 256), 0) // 32
    ib = lax.broadcasted_iota(jnp.int32, (256, 256), 1) // 32
    low = lax.broadcasted_iota(jnp.int32, (512, 128), 1) // 64

    def superblock(s):
        n = s // 2 + 1
        second = lax.rem(s, 2)
        h = 1 - second
        base = first_unit(n)

        @pl.when(second == 0)
        def _():
            loop(0, n, lambda j: p_land(base + j).wait_recv())

        gp_s[...] = jnp.zeros_like(gp_s)
        a_s[...] = jnp.zeros_like(a_s)
        q_s[...] = jnp.zeros_like(q_s)
        keep = low == h
        done = base + n + LAG + LEAD

        def gram(j):
            at = second * n + j

            @pl.when(n < 8)
            def _():
                loop(done + at * (n + 1) // (2 * n), done + (at + 1) * (n + 1) // (2 * n), comm)

            cols = []
            for xx in (0, 1):
                same = buf[h, xx, :, :, unit(base + j), :].reshape(512, 128)
                other = buf[1 - h, xx, :, :, unit(base + j), :].reshape(512, 128)
                cols.append(jnp.where(keep, same, pltpu.roll(other, 64, 1)))
            v = jnp.concatenate(cols, axis=1)
            vh, vm, vl = split3(v)
            rows = pl.ds(pl.multiple_of(j * 512, 512), 512)
            vh_s[rows, :] = vh
            vm_s[rows, :] = vm
            vl_s[rows, :] = vl
            th, tm, tl = split3(v.T)
            xh, xm, xl = split3(xbuf[8 - n + j].reshape(512, 128))
            x2 = jnp.concatenate([xh, xm], axis=1)
            gp_s[...] += bdot(
                jnp.concatenate([th, tm], axis=1),
                jnp.concatenate([jnp.concatenate([vh, x2], axis=1), jnp.concatenate([vm, x2], axis=1)], axis=0),
            )
            a_s[...] += bdot(jnp.concatenate([th, th], axis=1), jnp.concatenate([vm, vl], axis=0))
            q_s[...] += bdot(jnp.concatenate([tl, th], axis=1), jnp.concatenate([xh, xl], axis=0))

        loop(0, n, gram)

        a = a_s[...]
        g = gp_s[:, :256] + (a + a.T)
        w = (q_s[...] + gp_s[:, 384:]) + gp_s[:, 256:384]
        na = 4 * (ia % 2) + ia // 2
        nb = 4 * (ib % 2) + ib // 2
        diag = []
        t_rows = pl.ds(pl.multiple_of(32 * (8 - n), 32), 32)
        for xx in (0, 1):
            for cc in (0, 1):
                raw = tbuf[cc, xx, t_rows, :]
                e = jnp.where(h == cc, raw, pltpu.roll(raw, 64, 1))
                diag += [e, e]
        t4 = jnp.concatenate(diag, axis=0)
        t = jnp.where(ia == ib, jnp.concatenate([t4, t4], axis=1), 0.0)
        for lev in (1, 2, 4):
            pick = (na // (2 * lev) == nb // (2 * lev)) & ((na // lev) % 2 == 0) & ((nb // lev) % 2 == 1)
            t = t - fdot(fdot(t, jnp.where(pick, g, 0.0)), t)
        yh, ym, yl = split3(fdot(t, w))
        y2 = jnp.concatenate([yh, ym], axis=1)
        y22 = jnp.concatenate([y2, y2], axis=0)
        yq = jnp.concatenate([yh, yl], axis=0)

        def update(j):
            rows = pl.ds(pl.multiple_of(j * 512, 512), 512)
            vh = vh_s[rows, :]
            z2 = bdot(jnp.concatenate([vh, vm_s[rows, :]], axis=1), y22)
            zq = bdot(jnp.concatenate([vl_s[rows, :], vh], axis=1), yq)
            delta = (zq + z2[:, 128:]) + z2[:, :128]
            xbuf[8 - n + j] = xbuf[8 - n + j] - delta.reshape(2, 4, 64, 128)

        loop(0, n, update)

    loop(0, 16, superblock)

    def z_out(r):
        return pltpu.make_async_copy(xbuf.at[:, lax.rem(r, 2), r // 2], o_ref.at[r], in_sem.at[1])

    loop(0, 8, lambda r: z_out(r).start())

    remote(buf.at[c, x, y, 0:3], z_sem.at[0], x_dev, 0).wait_send()
    remote(buf.at[c, x, y], x1_sem.at[0], x_dev, 1).wait_send()
    remote(buf.at[c, x, y], y1_sem.at[0], y_dev, 2).wait_send()
    remote(buf.at[c, 1 - x, y, 0:2], y2_sem.at[0], y_dev, 3).wait_send()
    remote(buf.at[c, x, 1 - y, 2:4], x2_sem.at[0], x_dev, 4).wait_send()
    remote(buf.at[c], p_sem.at[0], p_dev, 5).wait_send()
    t_x.wait_send()
    t_p[0].wait_send()
    t_p[1].wait_send()
    pltpu.make_async_copy(xbuf, xbuf, in_sem.at[1]).wait()


def solution(mesh):
    def local_apply(v_loc, t_loc, z_loc):
        t2 = t_loc.reshape(8, 4, 32, 32).transpose(0, 2, 1, 3).reshape(256, 128)
        out = pl.pallas_call(
            fused_kernel,
            out_shape=jax.ShapeDtypeStruct((8, 8, 64, 128), F32),
            in_specs=[pl.BlockSpec(memory_space=pl.ANY)] * 3,
            out_specs=pl.BlockSpec(memory_space=pl.ANY),
            scratch_shapes=[
                pltpu.VMEM((2, 2, 2, 4, 64 * UNITS, 128), F32),
                pltpu.VMEM((2, 2, 256, 128), F32),
                pltpu.VMEM((8, 2, 4, 64, 128), F32),
                pltpu.VMEM((4096, 256), BF16),
                pltpu.VMEM((4096, 256), BF16),
                pltpu.VMEM((4096, 256), BF16),
                pltpu.VMEM((256, 512), F32),
                pltpu.VMEM((256, 256), F32),
                pltpu.VMEM((256, 128), F32),
                pltpu.SemaphoreType.DMA((3,)),
                pltpu.SemaphoreType.DMA((9,)),
                pltpu.SemaphoreType.DMA((UNITS,)),
                pltpu.SemaphoreType.DMA((UNITS,)),
                pltpu.SemaphoreType.DMA((UNITS,)),
                pltpu.SemaphoreType.DMA((UNITS,)),
                pltpu.SemaphoreType.DMA((UNITS,)),
                pltpu.SemaphoreType.DMA((UNITS,)),
                pltpu.SemaphoreType.DMA((3,)),
            ],
            compiler_params=pltpu.CompilerParams(
                collective_id=0, has_side_effects=True, vmem_limit_bytes=66 * 1000 * 1000
            ),
            name="gather_apply",
        )(v_loc, t2, z_loc.reshape(8, 8, 64, 128))
        return out.reshape(4096, 128)

    return jax.shard_map(
        local_apply,
        mesh=mesh,
        in_specs=(P("row", "col"), P("col", None, None), P(None, ("row", "col"))),
        out_specs=P(None, ("row", "col")),
        check_vma=False,
    )
```

```python
import functools
import jax
import jax.numpy as jnp
from jax import lax
from jax.experimental import pallas as pl
from jax.experimental.pallas import tpu as pltpu
from jax.sharding import PartitionSpec as P

F32 = jnp.float32
BF16 = jnp.bfloat16
HI = lax.Precision.HIGHEST
MESH = pl.DeviceIdType.MESH
UNITS = 36
Z_AHEAD = 6
D1 = 2
D2 = 1
D3 = 1
LAG = D1 + D2 + D3


def split3(v):
    h = v.astype(BF16)
    r = v - h.astype(F32)
    m = r.astype(BF16)
    l = (r - m.astype(F32)).astype(BF16)
    return h, m, l


def bdot(a, b):
    return jnp.dot(a, b, preferred_element_type=F32)


def fdot(a, b):
    return jnp.dot(a, b, precision=HI, preferred_element_type=F32)


def loop(lo, hi, body):
    def step(i, carry):
        body(i)
        return carry

    lax.fori_loop(lo, hi, step, 0)


def fused_kernel(
    v_ref, t_ref, z_ref, o_ref, buf, tbuf, xbuf, vh_s, vm_s, vl_s, gp_s, a_s, q_s,
    in_sem, send_sem, z_sem, x1_sem, y1_sem, x2_sem, y2_sem, z2_sem, p_sem, t_sem,
):
    row, col = lax.axis_index("row"), lax.axis_index("col")
    z, y = row // 2, lax.rem(row, 2)
    x, c = col // 2, lax.rem(col, 2)
    x_dev = (row, (1 - x) * 2 + c)
    y_dev = (z * 2 + 1 - y, col)
    p_dev = (row, x * 2 + 1 - c)
    low_z = lax.rem(z, 2)
    slot = 2 * low_z + z // 2
    z2_dev = ((z + 1 - 2 * low_z) * 2 + y, col)
    z_devs = [(lax.rem(z + k, 4) * 2 + y, col) for k in (1, 2, 3)]

    def unit(q):
        return pl.ds(pl.multiple_of(64 * q, 64), 64)

    def remote(view, recv, dev, kind):
        return pltpu.make_async_remote_copy(
            src_ref=view, dst_ref=view, send_sem=send_sem.at[kind], recv_sem=recv, device_id=dev, device_id_type=MESH
        )

    def z_copy(q, k):
        return remote(buf.at[c, x, y, slot, unit(q)], z_sem.at[q], z_devs[k], 0)

    def x1_copy(q):
        return remote(buf.at[c, x, y, :, unit(q)], x1_sem.at[q], x_dev, 1)

    def y1_copy(q):
        return remote(buf.at[c, x, y, :, unit(q)], y1_sem.at[q], y_dev, 2)

    def y2_copy(q):
        return remote(buf.at[c, 1 - x, y, 2 * low_z, unit(q)], y2_sem.at[q], y_dev, 3)

    def x2_copy(q):
        return remote(buf.at[c, x, 1 - y, 2 * low_z + 1, unit(q)], x2_sem.at[q], x_dev, 4)

    def z2_copy(q):
        return remote(buf.at[c, 1 - x, 1 - y, pl.ds(2 * low_z, 2), unit(q)], z2_sem.at[q], z2_dev, 9)

    def p_copy(q, xx, yy):
        return remote(buf.at[c, xx, yy, :, unit(q)], p_sem.at[q], p_dev, 5)

    def z_land(q):
        return remote(buf.at[c, x, y, 0:3, unit(q)], z_sem.at[q], x_dev, 0)

    def x1_land(q):
        return remote(buf.at[c, 1 - x, y, :, unit(q)], x1_sem.at[q], x_dev, 1)

    def y1_land(q):
        return remote(buf.at[c, x, 1 - y, :, unit(q)], y1_sem.at[q], y_dev, 2)

    def y2_land(q):
        return remote(buf.at[c, 1 - x, 1 - y, 2 * low_z, unit(q)], y2_sem.at[q], y_dev, 3)

    def x2_land(q):
        return remote(buf.at[c, 1 - x, 1 - y, 2 * low_z + 1, unit(q)], x2_sem.at[q], x_dev, 4)

    def z2_land(q):
        return remote(buf.at[c, 1 - x, 1 - y, pl.ds(2 - 2 * low_z, 2), unit(q)], z2_sem.at[q], z2_dev, 9)

    def p_land(q):
        return remote(buf.at[1 - c, :, :, :, unit(q)], p_sem.at[q], p_dev, 5)

    def z_send(q):
        for k in range(3):
            z_copy(q, k).start()

    def comm(q):
        @pl.when(q + Z_AHEAD < UNITS)
        def _():
            z_send(q + Z_AHEAD)

        @pl.when(q < UNITS)
        def _():
            z_land(q).wait_recv()
            x1_copy(q).start()
            y1_copy(q).start()
            p_copy(q, x, y).start()

        q1 = q - D1

        @pl.when((q1 >= 0) & (q1 < UNITS))
        def _():
            x1_land(q1).wait_recv()
            y2_copy(q1).start()
            y1_land(q1).wait_recv()
            x2_copy(q1).start()
            p_copy(q1, 1 - x, y).start()
            p_copy(q1, x, 1 - y).start()

        q2 = q - D1 - D2

        @pl.when((q2 >= 0) & (q2 < UNITS))
        def _():
            y2_land(q2).wait_recv()
            x2_land(q2).wait_recv()
            z2_copy(q2).start()

        q3 = q - LAG

        @pl.when((q3 >= 0) & (q3 < UNITS))
        def _():
            z2_land(q3).wait_recv()
            p_copy(q3, 1 - x, 1 - y).start()

    def first_unit(n):
        return n * (n - 1) // 2

    def v_in(n, j):
        src = v_ref.at[pl.ds(pl.multiple_of(64 * (8 - n + j), 64), 64), pl.ds(pl.multiple_of(128 * (8 - n), 128), 128)]
        return pltpu.make_async_copy(src, buf.at[c, x, y, slot, unit(first_unit(n) + j)], in_sem.at[0])

    def place(r):
        return 2 * lax.rem(r // 2, 2) + r // 4

    def z_in(r):
        return pltpu.make_async_copy(z_ref.at[r], xbuf.at[:, lax.rem(r, 2), place(r)], in_sem.at[1])

    t_in = pltpu.make_async_copy(t_ref, tbuf.at[c, x], in_sem.at[2])
    loop(1, 9, lambda n: loop(0, n, lambda j: v_in(n, j).start()))
    t_in.start()
    loop(0, 8, lambda r: z_in(r).start())

    barrier = pltpu.get_barrier_semaphore()
    for dev in [x_dev, y_dev, p_dev] + z_devs:
        pl.semaphore_signal(barrier, inc=1, device_id=dev, device_id_type=MESH)
    own = buf.at[c, x, y, slot]
    pltpu.make_async_copy(own, own, in_sem.at[0]).wait()
    pl.semaphore_wait(barrier, 6)

    loop(0, Z_AHEAD, z_send)
    t_in.wait()
    t_x = remote(tbuf.at[c, x], t_sem.at[0], x_dev, 6)
    t_p = [remote(tbuf.at[c, x], t_sem.at[1], p_dev, 7), remote(tbuf.at[c, 1 - x], t_sem.at[2], p_dev, 8)]
    t_x.start()
    t_p[0].start()
    loop(0, 1 + LAG, comm)
    remote(tbuf.at[c, 1 - x], t_sem.at[0], x_dev, 6).wait_recv()
    t_p[1].start()
    pltpu.make_async_copy(xbuf, xbuf, in_sem.at[1]).wait()
    remote(tbuf.at[1 - c, x], t_sem.at[1], p_dev, 7).wait_recv()
    remote(tbuf.at[1 - c, 1 - x], t_sem.at[2], p_dev, 8).wait_recv()

    ia = lax.broadcasted_iota(jnp.int32, (256, 256), 0) // 32
    ib = lax.broadcasted_iota(jnp.int32, (256, 256), 1) // 32
    low = lax.broadcasted_iota(jnp.int32, (512, 128), 1) // 64

    def steps(n):
        return first_unit(n) + LAG + n - (n - 1) // 2

    def superblock(s):
        n = s // 2 + 1
        second = lax.rem(s, 2)
        h = 1 - second
        base = first_unit(n)

        gp_s[...] = jnp.zeros_like(gp_s)
        a_s[...] = jnp.zeros_like(a_s)
        q_s[...] = jnp.zeros_like(q_s)
        keep = low == h

        def gram(j):
            at = second * n + j

            @pl.when(n < 8)
            def _():
                grow = steps(n + 1) - steps(n)
                loop(steps(n) + at * grow // (2 * n), steps(n) + (at + 1) * grow // (2 * n), comm)

            @pl.when((n == 8) & (second == 0))
            def _():
                grow = UNITS + LAG - steps(8)
                loop(steps(8) + j * grow // 8, steps(8) + (j + 1) * grow // 8, comm)

            @pl.when(second == 0)
            def _():
                p_land(base + j).wait_recv()

            cols = []
            for xx in (0, 1):
                same = buf[h, xx, :, :, unit(base + j), :].reshape(512, 128)
                other = buf[1 - h, xx, :, :, unit(base + j), :].reshape(512, 128)
                cols.append(jnp.where(keep, same, pltpu.roll(other, 64, 1)))
            v = jnp.concatenate(cols, axis=1)
            vh, vm, vl = split3(v)
            rows = pl.ds(pl.multiple_of(j * 512, 512), 512)
            vh_s[rows, :] = vh
            vm_s[rows, :] = vm
            vl_s[rows, :] = vl
            th, tm, tl = split3(v.T)
            xh, xm, xl = split3(xbuf[8 - n + j].reshape(512, 128))
            x2 = jnp.concatenate([xh, xm], axis=1)
            gp_s[...] += bdot(
                jnp.concatenate([th, tm], axis=1),
                jnp.concatenate([jnp.concatenate([vh, x2], axis=1), jnp.concatenate([vm, x2], axis=1)], axis=0),
            )
            a_s[...] += bdot(jnp.concatenate([th, th], axis=1), jnp.concatenate([vm, vl], axis=0))
            q_s[...] += bdot(jnp.concatenate([tl, th], axis=1), jnp.concatenate([xh, xl], axis=0))

        loop(0, n, gram)

        a = a_s[...]
        g = gp_s[:, :256] + (a + a.T)
        w = (q_s[...] + gp_s[:, 384:]) + gp_s[:, 256:384]
        na = 4 * (ia % 2) + ia // 2
        nb = 4 * (ib % 2) + ib // 2
        diag = []
        t_rows = pl.ds(pl.multiple_of(32 * (8 - n), 32), 32)
        for xx in (0, 1):
            for cc in (0, 1):
                raw = tbuf[cc, xx, t_rows, :]
                e = jnp.where(h == cc, raw, pltpu.roll(raw, 64, 1))
                diag += [e, e]
        t4 = jnp.concatenate(diag, axis=0)
        t = jnp.where(ia == ib, jnp.concatenate([t4, t4], axis=1), 0.0)
        for lev in (1, 2, 4):
            pick = (na // (2 * lev) == nb // (2 * lev)) & ((na // lev) % 2 == 0) & ((nb // lev) % 2 == 1)
            t = t - fdot(fdot(t, jnp.where(pick, g, 0.0)), t)
        yh, ym, yl = split3(fdot(t, w))
        y2 = jnp.concatenate([yh, ym], axis=1)
        y22 = jnp.concatenate([y2, y2], axis=0)
        yq = jnp.concatenate([yh, yl], axis=0)

        def update(j):
            rows = pl.ds(pl.multiple_of(j * 512, 512), 512)
            vh = vh_s[rows, :]
            z2 = bdot(jnp.concatenate([vh, vm_s[rows, :]], axis=1), y22)
            zq = bdot(jnp.concatenate([vl_s[rows, :], vh], axis=1), yq)
            delta = (zq + z2[:, 128:]) + z2[:, :128]
            xbuf[8 - n + j] = xbuf[8 - n + j] - delta.reshape(2, 4, 64, 128)

        loop(0, n, update)

    loop(0, 16, superblock)

    def z_out(r):
        return pltpu.make_async_copy(xbuf.at[:, lax.rem(r, 2), place(r)], o_ref.at[r], in_sem.at[1])

    loop(0, 8, lambda r: z_out(r).start())

    remote(buf.at[c, x, y, 0:3], z_sem.at[0], x_dev, 0).wait_send()
    remote(buf.at[c, x, y], x1_sem.at[0], x_dev, 1).wait_send()
    remote(buf.at[c, x, y], y1_sem.at[0], y_dev, 2).wait_send()
    remote(buf.at[c, 1 - x, y, 0], y2_sem.at[0], y_dev, 3).wait_send()
    remote(buf.at[c, x, 1 - y, 0], x2_sem.at[0], x_dev, 4).wait_send()
    remote(buf.at[c, 1 - x, 1 - y, 0:2], z2_sem.at[0], z2_dev, 9).wait_send()
    remote(buf.at[c], p_sem.at[0], p_dev, 5).wait_send()
    t_x.wait_send()
    t_p[0].wait_send()
    t_p[1].wait_send()
    pltpu.make_async_copy(xbuf, xbuf, in_sem.at[1]).wait()


def solution(mesh):
    def local_apply(v_loc, t_loc, z_loc):
        t2 = t_loc.reshape(8, 4, 32, 32).transpose(0, 2, 1, 3).reshape(256, 128)
        out = pl.pallas_call(
            fused_kernel,
            out_shape=jax.ShapeDtypeStruct((8, 8, 64, 128), F32),
            in_specs=[pl.BlockSpec(memory_space=pl.ANY)] * 3,
            out_specs=pl.BlockSpec(memory_space=pl.ANY),
            scratch_shapes=[
                pltpu.VMEM((2, 2, 2, 4, 64 * UNITS, 128), F32),
                pltpu.VMEM((2, 2, 256, 128), F32),
                pltpu.VMEM((8, 2, 4, 64, 128), F32),
                pltpu.VMEM((4096, 256), BF16),
                pltpu.VMEM((4096, 256), BF16),
                pltpu.VMEM((4096, 256), BF16),
                pltpu.VMEM((256, 512), F32),
                pltpu.VMEM((256, 256), F32),
                pltpu.VMEM((256, 128), F32),
                pltpu.SemaphoreType.DMA((3,)),
                pltpu.SemaphoreType.DMA((10,)),
                pltpu.SemaphoreType.DMA((UNITS,)),
                pltpu.SemaphoreType.DMA((UNITS,)),
                pltpu.SemaphoreType.DMA((UNITS,)),
                pltpu.SemaphoreType.DMA((UNITS,)),
                pltpu.SemaphoreType.DMA((UNITS,)),
                pltpu.SemaphoreType.DMA((UNITS,)),
                pltpu.SemaphoreType.DMA((UNITS,)),
                pltpu.SemaphoreType.DMA((3,)),
            ],
            compiler_params=pltpu.CompilerParams(
                collective_id=0, has_side_effects=True, vmem_limit_bytes=66 * 1000 * 1000
            ),
            name="gather_apply",
        )(v_loc, t2, z_loc.reshape(8, 8, 64, 128))
        return out.reshape(4096, 128)

    return jax.shard_map(
        local_apply,
        mesh=mesh,
        in_specs=(P("row", "col"), P("col", None, None), P(None, ("row", "col"))),
        out_specs=P(None, ("row", "col")),
        check_vma=False,
    )
```

```python
import functools
import jax
import jax.numpy as jnp
from jax import lax
from jax.experimental import pallas as pl
from jax.experimental.pallas import tpu as pltpu
from jax.sharding import PartitionSpec as P

F32 = jnp.float32
BF16 = jnp.bfloat16
HI = lax.Precision.HIGHEST
MESH = pl.DeviceIdType.MESH
UNITS = 36
Z_AHEAD = 6
D1 = 3
D2 = 2
D3 = 2
LAG = D1 + D2 + D3


def split3(v):
    h = v.astype(BF16)
    r = v - h.astype(F32)
    m = r.astype(BF16)
    l = (r - m.astype(F32)).astype(BF16)
    return h, m, l


def bdot(a, b):
    return jnp.dot(a, b, preferred_element_type=F32)


def ndot(a, b):
    return lax.dot_general(a, b, (((1,), (1,)), ((), ())), preferred_element_type=F32)


def fdot(a, b):
    return jnp.dot(a, b, precision=HI, preferred_element_type=F32)


def loop(lo, hi, body):
    def step(i, carry):
        body(i)
        return carry

    lax.fori_loop(lo, hi, step, 0)


def fused_kernel(
    v_ref, t_ref, z_ref, o_ref, buf, tbuf, stage, xt, tx, vh_s, vm_s, vl_s, g_s, a_s, w_s,
    in_sem, send_sem, z_sem, x1_sem, y1_sem, x2_sem, y2_sem, z2_sem, p_sem, t_sem, tx_sem,
):
    row, col = lax.axis_index("row"), lax.axis_index("col")
    z, y = row // 2, lax.rem(row, 2)
    x, c = col // 2, lax.rem(col, 2)
    x_dev = (row, (1 - x) * 2 + c)
    y_dev = (z * 2 + 1 - y, col)
    p_dev = (row, x * 2 + 1 - c)
    low_z = lax.rem(z, 2)
    slot = 2 * low_z + z // 2
    z2_dev = ((z + 1 - 2 * low_z) * 2 + y, col)
    z_devs = [(lax.rem(z + k, 4) * 2 + y, col) for k in (1, 2, 3)]

    def unit(q):
        return pl.ds(pl.multiple_of(64 * q, 64), 64)

    def remote(view, recv, dev, kind):
        return pltpu.make_async_remote_copy(
            src_ref=view, dst_ref=view, send_sem=send_sem.at[kind], recv_sem=recv, device_id=dev, device_id_type=MESH
        )

    def z_copy(q, k):
        return remote(buf.at[c, x, y, slot, unit(q)], z_sem.at[q], z_devs[k], 0)

    def x1_copy(q):
        return remote(buf.at[c, x, y, :, unit(q)], x1_sem.at[q], x_dev, 1)

    def y1_copy(q):
        return remote(buf.at[c, x, y, :, unit(q)], y1_sem.at[q], y_dev, 2)

    def y2_copy(q):
        return remote(buf.at[c, 1 - x, y, 2 * low_z, unit(q)], y2_sem.at[q], y_dev, 3)

    def x2_copy(q):
        return remote(buf.at[c, x, 1 - y, 2 * low_z + 1, unit(q)], x2_sem.at[q], x_dev, 4)

    def z2_copy(q):
        return remote(buf.at[c, 1 - x, 1 - y, pl.ds(2 * low_z, 2), unit(q)], z2_sem.at[q], z2_dev, 9)

    def p_copy(q, xx, yy):
        return remote(buf.at[c, xx, yy, :, unit(q)], p_sem.at[q], p_dev, 5)

    def z_land(q):
        return remote(buf.at[c, x, y, 0:3, unit(q)], z_sem.at[q], x_dev, 0)

    def x1_land(q):
        return remote(buf.at[c, 1 - x, y, :, unit(q)], x1_sem.at[q], x_dev, 1)

    def y1_land(q):
        return remote(buf.at[c, x, 1 - y, :, unit(q)], y1_sem.at[q], y_dev, 2)

    def y2_land(q):
        return remote(buf.at[c, 1 - x, 1 - y, 2 * low_z, unit(q)], y2_sem.at[q], y_dev, 3)

    def x2_land(q):
        return remote(buf.at[c, 1 - x, 1 - y, 2 * low_z + 1, unit(q)], x2_sem.at[q], x_dev, 4)

    def z2_land(q):
        return remote(buf.at[c, 1 - x, 1 - y, pl.ds(2 - 2 * low_z, 2), unit(q)], z2_sem.at[q], z2_dev, 9)

    def p_land(q):
        return remote(buf.at[1 - c, :, :, :, unit(q)], p_sem.at[q], p_dev, 5)

    def z_send(q):
        for k in range(3):
            z_copy(q, k).start()

    def comm(q):
        @pl.when(q + Z_AHEAD < UNITS)
        def _():
            z_send(q + Z_AHEAD)

        q1 = q - D1

        @pl.when((q1 >= 0) & (q1 < UNITS))
        def _():
            x1_land(q1).wait_recv()
            y2_copy(q1).start()
            y1_land(q1).wait_recv()
            x2_copy(q1).start()
            p_copy(q1, 1 - x, y).start()
            p_copy(q1, x, 1 - y).start()

        @pl.when(q < UNITS)
        def _():
            z_land(q).wait_recv()
            x1_copy(q).start()
            y1_copy(q).start()
            p_copy(q, x, y).start()

        q2 = q - D1 - D2

        @pl.when((q2 >= 0) & (q2 < UNITS))
        def _():
            y2_land(q2).wait_recv()
            x2_land(q2).wait_recv()
            z2_copy(q2).start()

        q3 = q - LAG

        @pl.when((q3 >= 0) & (q3 < UNITS))
        def _():
            z2_land(q3).wait_recv()
            p_copy(q3, 1 - x, 1 - y).start()

    def first_unit(n):
        return n * (n - 1) // 2

    def v_in(n, j):
        src = v_ref.at[pl.ds(pl.multiple_of(64 * (8 - n + j), 64), 64), pl.ds(pl.multiple_of(128 * (8 - n), 128), 128)]
        return pltpu.make_async_copy(src, buf.at[c, x, y, slot, unit(first_unit(n) + j)], in_sem.at[0])

    def place(r):
        return 2 * lax.rem(r // 2, 2) + r // 4

    def z_in(r):
        return pltpu.make_async_copy(z_ref.at[r], stage.at[:, lax.rem(r, 2), place(r)], in_sem.at[1])

    t_in = pltpu.make_async_copy(t_ref, tbuf.at[c, x], in_sem.at[2])
    loop(1, 9, lambda n: loop(0, n, lambda j: v_in(n, j).start()))
    t_in.start()
    loop(0, 8, lambda r: z_in(r).start())

    barrier = pltpu.get_barrier_semaphore()
    for dev in [x_dev, y_dev, p_dev] + z_devs:
        pl.semaphore_signal(barrier, inc=1, device_id=dev, device_id_type=MESH)
    own = buf.at[c, x, y, slot]
    pltpu.make_async_copy(own, own, in_sem.at[0]).wait()
    pl.semaphore_wait(barrier, 6)

    loop(0, Z_AHEAD, z_send)
    t_in.wait()
    t_x = remote(tbuf.at[c, x], t_sem.at[0], x_dev, 6)
    t_p = [remote(tbuf.at[c, x], t_sem.at[1], p_dev, 7), remote(tbuf.at[c, 1 - x], t_sem.at[2], p_dev, 8)]
    t_x.start()
    t_p[0].start()
    loop(0, 1 + LAG, comm)
    remote(tbuf.at[c, 1 - x], t_sem.at[0], x_dev, 6).wait_recv()
    t_p[1].start()
    pltpu.make_async_copy(stage, stage, in_sem.at[1]).wait()

    def turn_in(u):
        xt[u] = stage[u].reshape(512, 128).T

    loop(0, 8, turn_in)
    remote(tbuf.at[1 - c, x], t_sem.at[1], p_dev, 7).wait_recv()
    remote(tbuf.at[1 - c, 1 - x], t_sem.at[2], p_dev, 8).wait_recv()

    ia = lax.broadcasted_iota(jnp.int32, (256, 256), 0) // 32
    ib = lax.broadcasted_iota(jnp.int32, (256, 256), 1) // 32
    low = lax.broadcasted_iota(jnp.int32, (512, 128), 1) // 64

    def steps(n):
        return first_unit(n) + LAG + n - n // 4

    def share(n, at):
        grow = steps(n + 1) - steps(n)
        loop(steps(n) + at * grow // (3 * n), steps(n) + (at + 1) * grow // (3 * n), comm)

    def assemble(q, h):
        cols = []
        for xx in (0, 1):
            same = buf[h, xx, :, :, unit(q), :].reshape(512, 128)
            other = buf[1 - h, xx, :, :, unit(q), :].reshape(512, 128)
            cols.append(jnp.where(low == h, same, pltpu.roll(other, 64, 1)))
        return jnp.concatenate(cols, axis=1)

    def t_copy(n, half):
        return remote(tx.at[n - 1, half], tx_sem.at[n - 1], p_dev, 10)

    def pair(n):
        base = first_unit(n)
        g_s[...] = jnp.zeros_like(g_s)
        a_s[...] = jnp.zeros_like(a_s)

        def gram(j):
            @pl.when(n < 8)
            def _():
                share(n, j)

            @pl.when(n == 8)
            def _():
                grow = UNITS + LAG - steps(8)
                loop(steps(8) + j * grow // 8, steps(8) + (j + 1) * grow // 8, comm)

            p_land(base + j).wait_recv()
            v = assemble(base + j, c)
            vh, vm, vl = split3(v)
            th, tm, _ = split3(v.T)
            g_s[...] += bdot(jnp.concatenate([th, tm], axis=1), jnp.concatenate([vh, vm], axis=0))
            a_s[...] += bdot(jnp.concatenate([th, th], axis=1), jnp.concatenate([vm, vl], axis=0))

        loop(0, n, gram)

        a = a_s[...]
        g = g_s[...] + (a + a.T)
        na = 4 * (ia % 2) + ia // 2
        nb = 4 * (ib % 2) + ib // 2
        diag = []
        t_rows = pl.ds(pl.multiple_of(32 * (8 - n), 32), 32)
        for xx in (0, 1):
            for cc in (0, 1):
                raw = tbuf[cc, xx, t_rows, :]
                e = jnp.where(c == cc, raw, pltpu.roll(raw, 64, 1))
                diag += [e, e]
        t4 = jnp.concatenate(diag, axis=0)
        t = jnp.where(ia == ib, jnp.concatenate([t4, t4], axis=1), 0.0)
        for lev in (1, 2, 4):
            pick = (na // (2 * lev) == nb // (2 * lev)) & ((na // lev) % 2 == 0) & ((nb // lev) % 2 == 1)
            t = t - fdot(fdot(t, jnp.where(pick, g, 0.0)), t)
        tx[n - 1, c] = t.T
        t_copy(n, c).start()

        def half(second):
            h = 1 - second
            w_s[...] = jnp.zeros_like(w_s)

            def project(j):
                @pl.when(n < 8)
                def _():
                    share(n, (1 + second) * n + j)

                vh, vm, vl = split3(assemble(base + j, h))
                rows = pl.ds(pl.multiple_of(j * 512, 512), 512)
                vh_s[rows, :] = vh
                vm_s[rows, :] = vm
                vl_s[rows, :] = vl
                xh, xm, xl = split3(xt[8 - n + j])
                p1 = bdot(jnp.concatenate([xh, xm, xl], axis=0), vh)
                p2 = bdot(jnp.concatenate([xh, xm], axis=0), vm)
                p3 = bdot(xh, vl)
                w_s[...] += (((p3 + p1[256:]) + p2[128:]) + (p2[:128] + p1[128:256])) + p1[:128]

            loop(0, n, project)

            @pl.when(second == 0)
            def _():
                t_copy(n, 1 - c).wait_recv()

            yh, ym, yl = split3(fdot(w_s[...], tx[n - 1, h]))
            y2 = jnp.concatenate([yh, ym], axis=0)
            y3 = jnp.concatenate([yh, ym, yl], axis=0)

            def update(j):
                rows = pl.ds(pl.multiple_of(j * 512, 512), 512)
                d1 = ndot(y3, vh_s[rows, :])
                d2 = ndot(y2, vm_s[rows, :])
                d3 = ndot(yh, vl_s[rows, :])
                xt[8 - n + j] -= (((d3 + d1[256:]) + d2[128:]) + (d2[:128] + d1[128:256])) + d1[:128]

            loop(0, n, update)

        loop(0, 2, half)

    loop(1, 9, pair)

    def turn_out(u):
        stage[u] = xt[u].T.reshape(2, 4, 64, 128)

        def z_out(r):
            pltpu.make_async_copy(stage.at[u, lax.rem(r, 2), place(r)], o_ref.at[r, u], in_sem.at[1]).start()

        loop(0, 8, z_out)

    loop(0, 8, turn_out)

    remote(buf.at[c, x, y, 0:3], z_sem.at[0], x_dev, 0).wait_send()
    remote(buf.at[c, x, y], x1_sem.at[0], x_dev, 1).wait_send()
    remote(buf.at[c, x, y], y1_sem.at[0], y_dev, 2).wait_send()
    remote(buf.at[c, 1 - x, y, 0], y2_sem.at[0], y_dev, 3).wait_send()
    remote(buf.at[c, x, 1 - y, 0], x2_sem.at[0], x_dev, 4).wait_send()
    remote(buf.at[c, 1 - x, 1 - y, 0:2], z2_sem.at[0], z2_dev, 9).wait_send()
    remote(buf.at[c], p_sem.at[0], p_dev, 5).wait_send()
    t_x.wait_send()
    t_p[0].wait_send()
    t_p[1].wait_send()
    remote(tx.at[:, 0], tx_sem.at[0], p_dev, 10).wait_send()
    pltpu.make_async_copy(stage, stage, in_sem.at[1]).wait()


def solution(mesh):
    def local_apply(v_loc, t_loc, z_loc):
        t2 = t_loc.reshape(8, 4, 32, 32).transpose(0, 2, 1, 3).reshape(256, 128)
        out = pl.pallas_call(
            fused_kernel,
            out_shape=jax.ShapeDtypeStruct((8, 8, 64, 128), F32),
            in_specs=[pl.BlockSpec(memory_space=pl.ANY)] * 3,
            out_specs=pl.BlockSpec(memory_space=pl.ANY),
            scratch_shapes=[
                pltpu.VMEM((2, 2, 2, 4, 64 * UNITS, 128), F32),
                pltpu.VMEM((2, 2, 256, 128), F32),
                pltpu.VMEM((8, 2, 4, 64, 128), F32),
                pltpu.VMEM((8, 128, 512), F32),
                pltpu.VMEM((8, 2, 256, 256), F32),
                pltpu.VMEM((4096, 256), BF16),
                pltpu.VMEM((4096, 256), BF16),
                pltpu.VMEM((4096, 256), BF16),
                pltpu.VMEM((256, 256), F32),
                pltpu.VMEM((256, 256), F32),
                pltpu.VMEM((128, 256), F32),
                pltpu.SemaphoreType.DMA((3,)),
                pltpu.SemaphoreType.DMA((11,)),
                pltpu.SemaphoreType.DMA((UNITS,)),
                pltpu.SemaphoreType.DMA((UNITS,)),
                pltpu.SemaphoreType.DMA((UNITS,)),
                pltpu.SemaphoreType.DMA((UNITS,)),
                pltpu.SemaphoreType.DMA((UNITS,)),
                pltpu.SemaphoreType.DMA((UNITS,)),
                pltpu.SemaphoreType.DMA((UNITS,)),
                pltpu.SemaphoreType.DMA((3,)),
                pltpu.SemaphoreType.DMA((8,)),
            ],
            compiler_params=pltpu.CompilerParams(
                collective_id=0, has_side_effects=True, vmem_limit_bytes=66 * 1000 * 1000
            ),
            name="gather_apply",
        )(v_loc, t2, z_loc.reshape(8, 8, 64, 128))
        return out.reshape(4096, 128)

    return jax.shard_map(
        local_apply,
        mesh=mesh,
        in_specs=(P("row", "col"), P("col", None, None), P(None, ("row", "col"))),
        out_specs=P(None, ("row", "col")),
        check_vma=False,
    )
```

```python
import functools
import jax
import jax.numpy as jnp
from jax import lax
from jax.experimental import pallas as pl
from jax.experimental.pallas import tpu as pltpu
from jax.sharding import PartitionSpec as P

F32 = jnp.float32
BF16 = jnp.bfloat16
HI = lax.Precision.HIGHEST
MESH = pl.DeviceIdType.MESH
UNITS = 36
Z_AHEAD = 6
D1 = 2
D2 = 1
D3 = 1
LAG = D1 + D2 + D3


def split3(v):
    h = v.astype(BF16)
    r = v - h.astype(F32)
    m = r.astype(BF16)
    l = (r - m.astype(F32)).astype(BF16)
    return h, m, l


def bdot(a, b):
    return jnp.dot(a, b, preferred_element_type=F32)


def ndot(a, b):
    return lax.dot_general(a, b, (((1,), (1,)), ((), ())), preferred_element_type=F32)


def fdot(a, b):
    return jnp.dot(a, b, precision=HI, preferred_element_type=F32)


def loop(lo, hi, body):
    def step(i, carry):
        body(i)
        return carry

    lax.fori_loop(lo, hi, step, 0)


def fused_kernel(
    v_ref, t_ref, z_ref, o_ref, buf, traw, tbuf, stage, xt, tx, vh_s, vm_s, vl_s, g_s, a_s, w_s,
    in_sem, send_sem, z_sem, x1_sem, y1_sem, x2_sem, y2_sem, z2_sem, p_sem, t_sem, tx_sem,
):
    row, col = lax.axis_index("row"), lax.axis_index("col")
    z, y = row // 2, lax.rem(row, 2)
    x, c = col // 2, lax.rem(col, 2)
    x_dev = (row, (1 - x) * 2 + c)
    y_dev = (z * 2 + 1 - y, col)
    p_dev = (row, x * 2 + 1 - c)
    low_z = lax.rem(z, 2)
    slot = 2 * low_z + z // 2
    z2_dev = ((z + 1 - 2 * low_z) * 2 + y, col)
    z_devs = [(lax.rem(z + k, 4) * 2 + y, col) for k in (1, 2, 3)]

    def unit(q):
        return pl.ds(pl.multiple_of(64 * q, 64), 64)

    def remote(view, recv, dev, kind):
        return pltpu.make_async_remote_copy(
            src_ref=view, dst_ref=view, send_sem=send_sem.at[kind], recv_sem=recv, device_id=dev, device_id_type=MESH
        )

    def z_copy(q, k):
        return remote(buf.at[c, x, y, slot, unit(q)], z_sem.at[q], z_devs[k], 0)

    def x1_copy(q):
        return remote(buf.at[c, x, y, :, unit(q)], x1_sem.at[q], x_dev, 1)

    def y1_copy(q):
        return remote(buf.at[c, x, y, :, unit(q)], y1_sem.at[q], y_dev, 2)

    def y2_copy(q):
        return remote(buf.at[c, 1 - x, y, 2 * low_z, unit(q)], y2_sem.at[q], y_dev, 3)

    def x2_copy(q):
        return remote(buf.at[c, x, 1 - y, 2 * low_z + 1, unit(q)], x2_sem.at[q], x_dev, 4)

    def z2_copy(q):
        return remote(buf.at[c, 1 - x, 1 - y, pl.ds(2 * low_z, 2), unit(q)], z2_sem.at[q], z2_dev, 9)

    def p_copy(q, xx, yy):
        return remote(buf.at[c, xx, yy, :, unit(q)], p_sem.at[q], p_dev, 5)

    def z_land(q):
        return remote(buf.at[c, x, y, 0:3, unit(q)], z_sem.at[q], x_dev, 0)

    def x1_land(q):
        return remote(buf.at[c, 1 - x, y, :, unit(q)], x1_sem.at[q], x_dev, 1)

    def y1_land(q):
        return remote(buf.at[c, x, 1 - y, :, unit(q)], y1_sem.at[q], y_dev, 2)

    def y2_land(q):
        return remote(buf.at[c, 1 - x, 1 - y, 2 * low_z, unit(q)], y2_sem.at[q], y_dev, 3)

    def x2_land(q):
        return remote(buf.at[c, 1 - x, 1 - y, 2 * low_z + 1, unit(q)], x2_sem.at[q], x_dev, 4)

    def z2_land(q):
        return remote(buf.at[c, 1 - x, 1 - y, pl.ds(2 - 2 * low_z, 2), unit(q)], z2_sem.at[q], z2_dev, 9)

    def p_land(q):
        return remote(buf.at[1 - c, :, :, :, unit(q)], p_sem.at[q], p_dev, 5)

    def z_send(q):
        for k in range(3):
            z_copy(q, k).start()

    def comm(q):
        @pl.when(q + Z_AHEAD < UNITS)
        def _():
            z_send(q + Z_AHEAD)

        q1 = q - D1

        @pl.when((q1 >= 0) & (q1 < UNITS))
        def _():
            x1_land(q1).wait_recv()
            y2_copy(q1).start()
            y1_land(q1).wait_recv()
            x2_copy(q1).start()
            p_copy(q1, 1 - x, y).start()
            p_copy(q1, x, 1 - y).start()

        @pl.when(q < UNITS)
        def _():
            z_land(q).wait_recv()
            x1_copy(q).start()
            y1_copy(q).start()
            p_copy(q, x, y).start()

        q2 = q - D1 - D2

        @pl.when((q2 >= 0) & (q2 < UNITS))
        def _():
            y2_land(q2).wait_recv()
            x2_land(q2).wait_recv()
            z2_copy(q2).start()

        q3 = q - LAG

        @pl.when((q3 >= 0) & (q3 < UNITS))
        def _():
            z2_land(q3).wait_recv()
            p_copy(q3, 1 - x, 1 - y).start()

    def first_unit(n):
        return n * (n - 1) // 2

    def v_in(n, j):
        src = v_ref.at[pl.ds(pl.multiple_of(64 * (8 - n + j), 64), 64), pl.ds(pl.multiple_of(128 * (8 - n), 128), 128)]
        return pltpu.make_async_copy(src, buf.at[c, x, y, slot, unit(first_unit(n) + j)], in_sem.at[0])

    def place(r):
        return 2 * lax.rem(r // 2, 2) + r // 4

    def z_in(r):
        return pltpu.make_async_copy(z_ref.at[r], stage.at[:, lax.rem(r, 2), place(r)], in_sem.at[1])

    t_in = pltpu.make_async_copy(t_ref, traw, in_sem.at[2])
    loop(1, 9, lambda n: loop(0, n, lambda j: v_in(n, j).start()))
    t_in.start()
    loop(0, 8, lambda r: z_in(r).start())

    barrier = pltpu.get_barrier_semaphore()
    for dev in [x_dev, y_dev, p_dev] + z_devs:
        pl.semaphore_signal(barrier, inc=1, device_id=dev, device_id_type=MESH)
    own = buf.at[c, x, y, slot]
    pltpu.make_async_copy(own, own, in_sem.at[0]).wait()
    pl.semaphore_wait(barrier, 6)

    loop(0, Z_AHEAD, z_send)
    t_in.wait()

    def pack_t(b):
        rows = pl.ds(pl.multiple_of(32 * b, 32), 32)
        tbuf[c, x, rows, :] = jnp.concatenate([traw[4 * b + k] for k in range(4)], axis=1)

    loop(0, 8, pack_t)
    loop(0, 2, comm)
    t_x = remote(tbuf.at[c, x], t_sem.at[0], x_dev, 6)
    t_p = [remote(tbuf.at[c, x], t_sem.at[1], p_dev, 7), remote(tbuf.at[c, 1 - x], t_sem.at[2], p_dev, 8)]
    t_x.start()
    t_p[0].start()
    loop(2, 1 + LAG, comm)
    remote(tbuf.at[c, 1 - x], t_sem.at[0], x_dev, 6).wait_recv()
    t_p[1].start()
    pltpu.make_async_copy(stage, stage, in_sem.at[1]).wait()

    def turn_in(u):
        xt[u] = stage[u].reshape(512, 128).T

    loop(0, 8, turn_in)
    remote(tbuf.at[1 - c, x], t_sem.at[1], p_dev, 7).wait_recv()
    remote(tbuf.at[1 - c, 1 - x], t_sem.at[2], p_dev, 8).wait_recv()

    ia = lax.broadcasted_iota(jnp.int32, (256, 256), 0) // 32
    ib = lax.broadcasted_iota(jnp.int32, (256, 256), 1) // 32
    low = lax.broadcasted_iota(jnp.int32, (512, 128), 1) // 64

    def steps(n):
        return first_unit(n) + LAG + n - n // 4 - 2 * (n // 8)

    def share(n, at):
        grow = steps(n + 1) - steps(n)
        loop(steps(n) + at * grow // (4 * n), steps(n) + (at + 1) * grow // (4 * n), comm)

    def assemble(q, h):
        cols = []
        for xx in (0, 1):
            same = buf[h, xx, :, :, unit(q), :].reshape(512, 128)
            other = buf[1 - h, xx, :, :, unit(q), :].reshape(512, 128)
            cols.append(jnp.where(low == h, same, pltpu.roll(other, 64, 1)))
        return jnp.concatenate(cols, axis=1)

    def t_copy(n, half):
        return remote(tx.at[n - 1, half], tx_sem.at[n - 1], p_dev, 10)

    def pair(n):
        base = first_unit(n)
        g_s[...] = jnp.zeros_like(g_s)
        a_s[...] = jnp.zeros_like(a_s)
        w_s[...] = jnp.zeros_like(w_s)

        def apply_v(j, h):
            vh, vm, vl = split3(assemble(base + j, h))
            rows = pl.ds(pl.multiple_of(j * 512, 512), 512)
            vh_s[rows, :] = vh
            vm_s[rows, :] = vm
            vl_s[rows, :] = vl
            xh, xm, xl = split3(xt[8 - n + j])
            p1 = bdot(jnp.concatenate([xh, xm, xl], axis=0), vh)
            p2 = bdot(jnp.concatenate([xh, xm], axis=0), vm)
            p3 = bdot(xh, vl)
            w_s[...] += (((p3 + p1[256:]) + p2[128:]) + (p2[:128] + p1[128:256])) + p1[:128]

        def project(j):
            @pl.when(n < 8)
            def _():
                share(n, 2 * n + j)

            apply_v(j, 0)

        def gram(j):
            @pl.when(n < 8)
            def _():
                share(n, j)

            @pl.when(n == 8)
            def _():
                grow = UNITS + LAG - steps(8)
                loop(steps(8) + j * grow // 8, steps(8) + (j + 1) * grow // 8, comm)

            p_land(base + j).wait_recv()
            v = assemble(base + j, c)
            vh, vm, vl = split3(v)
            th, tm, _ = split3(v.T)
            g_s[...] += bdot(jnp.concatenate([th, tm], axis=1), jnp.concatenate([vh, vm], axis=0))
            a_s[...] += bdot(jnp.concatenate([th, th], axis=1), jnp.concatenate([vm, vl], axis=0))
            apply_v(j, 1)

        loop(0, n, gram)

        a = a_s[...]
        g = g_s[...] + (a + a.T)
        na = 4 * (ia % 2) + ia // 2
        nb = 4 * (ib % 2) + ib // 2
        diag = []
        t_rows = pl.ds(pl.multiple_of(32 * (8 - n), 32), 32)
        for xx in (0, 1):
            for cc in (0, 1):
                raw = tbuf[cc, xx, t_rows, :]
                e = jnp.where(c == cc, raw, pltpu.roll(raw, 64, 1))
                diag += [e, e]
        t4 = jnp.concatenate(diag, axis=0)
        t = jnp.where(ia == ib, jnp.concatenate([t4, t4], axis=1), 0.0)
        for lev in (1, 2, 4):
            pick = (na // (2 * lev) == nb // (2 * lev)) & ((na // lev) % 2 == 0) & ((nb // lev) % 2 == 1)
            t = t - fdot(fdot(t, jnp.where(pick, g, 0.0)), t)
        tx[n - 1, c] = t.T
        t_copy(n, c).start()

        def half(second):
            h = 1 - second

            @pl.when(second == 1)
            def _():
                w_s[...] = jnp.zeros_like(w_s)
                loop(0, n, project)

            @pl.when(second == 0)
            def _():
                t_copy(n, 1 - c).wait_recv()

            yh, ym, yl = split3(fdot(w_s[...], tx[n - 1, h]))
            y2 = jnp.concatenate([yh, ym], axis=0)
            y3 = jnp.concatenate([yh, ym, yl], axis=0)

            def update(j):
                @pl.when(n < 8)
                def _():
                    share(n, (1 + 2 * second) * n + j)

                rows = pl.ds(pl.multiple_of(j * 512, 512), 512)
                d1 = ndot(y3, vh_s[rows, :])
                d2 = ndot(y2, vm_s[rows, :])
                d3 = ndot(yh, vl_s[rows, :])
                xt[8 - n + j] -= (((d3 + d1[256:]) + d2[128:]) + (d2[:128] + d1[128:256])) + d1[:128]

            loop(0, n, update)

        loop(0, 2, half)

    loop(1, 9, pair)

    def turn_out(u):
        stage[u] = xt[u].T.reshape(2, 4, 64, 128)

        def z_out(r):
            pltpu.make_async_copy(stage.at[u, lax.rem(r, 2), place(r)], o_ref.at[r, u], in_sem.at[1]).start()

        loop(0, 8, z_out)

    loop(0, 8, turn_out)

    remote(buf.at[c, x, y, 0:3], z_sem.at[0], x_dev, 0).wait_send()
    remote(buf.at[c, x, y], x1_sem.at[0], x_dev, 1).wait_send()
    remote(buf.at[c, x, y], y1_sem.at[0], y_dev, 2).wait_send()
    remote(buf.at[c, 1 - x, y, 0], y2_sem.at[0], y_dev, 3).wait_send()
    remote(buf.at[c, x, 1 - y, 0], x2_sem.at[0], x_dev, 4).wait_send()
    remote(buf.at[c, 1 - x, 1 - y, 0:2], z2_sem.at[0], z2_dev, 9).wait_send()
    remote(buf.at[c], p_sem.at[0], p_dev, 5).wait_send()
    t_x.wait_send()
    t_p[0].wait_send()
    t_p[1].wait_send()
    remote(tx.at[:, 0], tx_sem.at[0], p_dev, 10).wait_send()
    pltpu.make_async_copy(stage, stage, in_sem.at[1]).wait()


def solution(mesh):
    def local_apply(v_loc, t_loc, z_loc):
        out = pl.pallas_call(
            fused_kernel,
            out_shape=jax.ShapeDtypeStruct((8, 8, 64, 128), F32),
            in_specs=[pl.BlockSpec(memory_space=pl.ANY)] * 3,
            out_specs=pl.BlockSpec(memory_space=pl.ANY),
            scratch_shapes=[
                pltpu.VMEM((2, 2, 2, 4, 64 * UNITS, 128), F32),
                pltpu.VMEM((32, 32, 32), F32),
                pltpu.VMEM((2, 2, 256, 128), F32),
                pltpu.VMEM((8, 2, 4, 64, 128), F32),
                pltpu.VMEM((8, 128, 512), F32),
                pltpu.VMEM((8, 2, 256, 256), F32),
                pltpu.VMEM((4096, 256), BF16),
                pltpu.VMEM((4096, 256), BF16),
                pltpu.VMEM((4096, 256), BF16),
                pltpu.VMEM((256, 256), F32),
                pltpu.VMEM((256, 256), F32),
                pltpu.VMEM((128, 256), F32),
                pltpu.SemaphoreType.DMA((3,)),
                pltpu.SemaphoreType.DMA((11,)),
                pltpu.SemaphoreType.DMA((UNITS,)),
                pltpu.SemaphoreType.DMA((UNITS,)),
                pltpu.SemaphoreType.DMA((UNITS,)),
                pltpu.SemaphoreType.DMA((UNITS,)),
                pltpu.SemaphoreType.DMA((UNITS,)),
                pltpu.SemaphoreType.DMA((UNITS,)),
                pltpu.SemaphoreType.DMA((UNITS,)),
                pltpu.SemaphoreType.DMA((3,)),
                pltpu.SemaphoreType.DMA((8,)),
            ],
            compiler_params=pltpu.CompilerParams(
                collective_id=0, has_side_effects=True, vmem_limit_bytes=66 * 1000 * 1000
            ),
            name="gather_apply",
        )(v_loc, t_loc, z_loc.reshape(8, 8, 64, 128))
        return out.reshape(4096, 128)

    return jax.shard_map(
        local_apply,
        mesh=mesh,
        in_specs=(P("row", "col"), P("col", None, None), P(None, ("row", "col"))),
        out_specs=P(None, ("row", "col")),
        check_vma=False,
    )
```

```python
import functools
import jax
import jax.numpy as jnp
from jax import lax
from jax.experimental import pallas as pl
from jax.experimental.pallas import tpu as pltpu
from jax.sharding import PartitionSpec as P

F32 = jnp.float32
BF16 = jnp.bfloat16
HI = lax.Precision.HIGHEST
MESH = pl.DeviceIdType.MESH
UNITS = 36
Z_AHEAD = 4
EARLY = 6
D1 = 3
D2 = 2
D3 = 3
LAG = D1 + D2 + D3


def split3(v):
    h = v.astype(BF16)
    r = v - h.astype(F32)
    m = r.astype(BF16)
    l = (r - m.astype(F32)).astype(BF16)
    return h, m, l


def bdot(a, b):
    return jnp.dot(a, b, preferred_element_type=F32)


def ndot(a, b):
    return lax.dot_general(a, b, (((1,), (1,)), ((), ())), preferred_element_type=F32)


def fdot(a, b):
    return jnp.dot(a, b, precision=HI, preferred_element_type=F32)


def loop(lo, hi, body):
    def step(i, carry):
        body(i)
        return carry

    lax.fori_loop(lo, hi, step, 0)


def fused_kernel(
    v_ref, t_ref, z_ref, o_ref, buf, traw, tbuf, stage, xt, tx, vh_s, vm_s, vl_s, g_s, a_s, w_s, y_s,
    in_sem, send_sem, z_sem, x1_sem, y1_sem, x2_sem, y2_sem, z2_sem, p_sem, t_sem, tx_sem,
):
    row, col = lax.axis_index("row"), lax.axis_index("col")
    z, y = row // 2, lax.rem(row, 2)
    x, c = col // 2, lax.rem(col, 2)
    x_dev = (row, (1 - x) * 2 + c)
    y_dev = (z * 2 + 1 - y, col)
    p_dev = (row, x * 2 + 1 - c)
    low_z = lax.rem(z, 2)
    slot = 2 * low_z + z // 2
    z2_dev = ((z + 1 - 2 * low_z) * 2 + y, col)
    z_devs = [(lax.rem(z + k, 4) * 2 + y, col) for k in (1, 2, 3)]

    def unit(q):
        return pl.ds(pl.multiple_of(64 * q, 64), 64)

    def remote(view, recv, dev, kind):
        return pltpu.make_async_remote_copy(
            src_ref=view, dst_ref=view, send_sem=send_sem.at[kind], recv_sem=recv, device_id=dev, device_id_type=MESH
        )

    def z_copy(q, k):
        return remote(buf.at[c, x, y, slot, unit(q)], z_sem.at[q], z_devs[k], 0)

    def x1_copy(q):
        return remote(buf.at[c, x, y, :, unit(q)], x1_sem.at[q], x_dev, 1)

    def y1_copy(q):
        return remote(buf.at[c, x, y, :, unit(q)], y1_sem.at[q], y_dev, 2)

    def xy_piece(q, k):
        view = buf.at[c, x, y, lax.rem(slot + k, 4), unit(q)]
        return remote(view, x1_sem.at[q], x_dev, 1), remote(view, y1_sem.at[q], y_dev, 2)

    def y2_copy(q):
        return remote(buf.at[c, 1 - x, y, 2 * low_z, unit(q)], y2_sem.at[q], y_dev, 3)

    def x2_copy(q):
        return remote(buf.at[c, x, 1 - y, 2 * low_z + 1, unit(q)], x2_sem.at[q], x_dev, 4)

    def z2_copy(q):
        return remote(buf.at[c, 1 - x, 1 - y, pl.ds(2 * low_z, 2), unit(q)], z2_sem.at[q], z2_dev, 9)

    def p_copy(q, xx, yy):
        return remote(buf.at[c, xx, yy, :, unit(q)], p_sem.at[q], p_dev, 5)

    def z_land(q):
        return remote(buf.at[c, x, y, 0:3, unit(q)], z_sem.at[q], x_dev, 0)

    def x1_land(q):
        return remote(buf.at[c, 1 - x, y, :, unit(q)], x1_sem.at[q], x_dev, 1)

    def y1_land(q):
        return remote(buf.at[c, x, 1 - y, :, unit(q)], y1_sem.at[q], y_dev, 2)

    def y2_land(q):
        return remote(buf.at[c, 1 - x, 1 - y, 2 * low_z, unit(q)], y2_sem.at[q], y_dev, 3)

    def x2_land(q):
        return remote(buf.at[c, 1 - x, 1 - y, 2 * low_z + 1, unit(q)], x2_sem.at[q], x_dev, 4)

    def z2_land(q):
        return remote(buf.at[c, 1 - x, 1 - y, pl.ds(2 - 2 * low_z, 2), unit(q)], z2_sem.at[q], z2_dev, 9)

    def p_land(q):
        return remote(buf.at[1 - c, :, :, :, unit(q)], p_sem.at[q], p_dev, 5)

    def z_send(q):
        for k in range(3):
            z_copy(q, k).start()

    def comm(q):
        @pl.when(q + Z_AHEAD < UNITS)
        def _():
            z_send(q + Z_AHEAD)

        q1 = q - D1

        @pl.when((q1 >= 0) & (q1 < UNITS))
        def _():
            x1_land(q1).wait_recv()
            y2_copy(q1).start()
            y1_land(q1).wait_recv()
            x2_copy(q1).start()
            p_copy(q1, 1 - x, y).start()
            p_copy(q1, x, 1 - y).start()

        @pl.when(q < UNITS)
        def _():
            z_land(q).wait_recv()

            @pl.when(q < EARLY)
            def _():
                for k in (1, 2, 3):
                    for copy in xy_piece(q, k):
                        copy.start()

            @pl.when(q >= EARLY)
            def _():
                x1_copy(q).start()
                y1_copy(q).start()

            p_copy(q, x, y).start()

        q2 = q - D1 - D2

        @pl.when((q2 >= 0) & (q2 < UNITS))
        def _():
            y2_land(q2).wait_recv()
            x2_land(q2).wait_recv()
            z2_copy(q2).start()

        q3 = q - LAG

        @pl.when((q3 >= 0) & (q3 < UNITS))
        def _():
            z2_land(q3).wait_recv()
            p_copy(q3, 1 - x, 1 - y).start()

    def first_unit(n):
        return n * (n - 1) // 2

    def v_in(n, j):
        src = v_ref.at[pl.ds(pl.multiple_of(64 * (8 - n + j), 64), 64), pl.ds(pl.multiple_of(128 * (8 - n), 128), 128)]
        return pltpu.make_async_copy(src, buf.at[c, x, y, slot, unit(first_unit(n) + j)], in_sem.at[0])

    def place(r):
        return 2 * lax.rem(r // 2, 2) + r // 4

    def z_in(r):
        return pltpu.make_async_copy(z_ref.at[r], stage.at[:, lax.rem(r, 2), place(r)], in_sem.at[1])

    t_in = pltpu.make_async_copy(t_ref, traw, in_sem.at[2])
    loop(1, 9, lambda n: loop(0, n, lambda j: v_in(n, j).start()))
    t_in.start()
    loop(0, 8, lambda r: z_in(r).start())

    barrier = pltpu.get_barrier_semaphore()
    for dev in [x_dev, y_dev, p_dev] + z_devs:
        pl.semaphore_signal(barrier, inc=1, device_id=dev, device_id_type=MESH)
    own = buf.at[c, x, y, slot]
    pltpu.make_async_copy(own, own, in_sem.at[0]).wait()
    pl.semaphore_wait(barrier, 6)

    loop(0, Z_AHEAD, z_send)

    def early(q):
        for copy in xy_piece(q, 0):
            copy.start()

    loop(0, EARLY, early)
    t_in.wait()

    def pack_t(b):
        rows = pl.ds(pl.multiple_of(32 * b, 32), 32)
        tbuf[c, x, rows, :] = jnp.concatenate([traw[4 * b + k] for k in range(4)], axis=1)

    loop(0, 8, pack_t)
    loop(0, 2, comm)
    t_x = remote(tbuf.at[c, x], t_sem.at[0], x_dev, 6)
    t_p = [remote(tbuf.at[c, x], t_sem.at[1], p_dev, 7), remote(tbuf.at[c, 1 - x], t_sem.at[2], p_dev, 8)]
    t_x.start()
    t_p[0].start()
    loop(2, 1 + LAG, comm)
    remote(tbuf.at[c, 1 - x], t_sem.at[0], x_dev, 6).wait_recv()
    t_p[1].start()
    pltpu.make_async_copy(stage, stage, in_sem.at[1]).wait()

    def turn_in(u):
        xt[u] = stage[u].reshape(512, 128).T

    loop(0, 8, turn_in)
    remote(tbuf.at[1 - c, x], t_sem.at[1], p_dev, 7).wait_recv()
    remote(tbuf.at[1 - c, 1 - x], t_sem.at[2], p_dev, 8).wait_recv()

    ia = lax.broadcasted_iota(jnp.int32, (256, 256), 0) // 32
    ib = lax.broadcasted_iota(jnp.int32, (256, 256), 1) // 32
    low = lax.broadcasted_iota(jnp.int32, (512, 128), 1) // 64

    def steps(n):
        return first_unit(n) + LAG + n - n // 4 - 2 * (n // 8)

    def share(n, at):
        grow = steps(n + 1) - steps(n)
        loop(steps(n) + at * grow // (3 * n), steps(n) + (at + 1) * grow // (3 * n), comm)

    def assemble(q, h):
        cols = []
        for xx in (0, 1):
            same = buf[h, xx, :, :, unit(q), :].reshape(512, 128)
            other = buf[1 - h, xx, :, :, unit(q), :].reshape(512, 128)
            cols.append(jnp.where(low == h, same, pltpu.roll(other, 64, 1)))
        return jnp.concatenate(cols, axis=1)

    def t_copy(n, half):
        return remote(tx.at[n - 1, half], tx_sem.at[n - 1], p_dev, 10)

    def pair(n):
        base = first_unit(n)
        g_s[...] = jnp.zeros_like(g_s)
        a_s[...] = jnp.zeros_like(a_s)
        w_s[...] = jnp.zeros_like(w_s)

        def apply_v(j, h):
            vh, vm, vl = split3(assemble(base + j, h))
            rows = pl.ds(pl.multiple_of(j * 512, 512), 512)
            vh_s[rows, :] = vh
            vm_s[rows, :] = vm
            vl_s[rows, :] = vl
            xh, xm, xl = split3(xt[8 - n + j])
            p1 = bdot(jnp.concatenate([xh, xm, xl], axis=0), vh)
            p2 = bdot(jnp.concatenate([xh, xm], axis=0), vm)
            p3 = bdot(xh, vl)
            w_s[...] += (((p3 + p1[256:]) + p2[128:]) + (p2[:128] + p1[128:256])) + p1[:128]

        def gram(j):
            @pl.when(n < 8)
            def _():
                share(n, j)

            @pl.when(n == 8)
            def _():
                grow = UNITS + LAG - steps(8)
                loop(steps(8) + j * grow // 8, steps(8) + (j + 1) * grow // 8, comm)

            p_land(base + j).wait_recv()
            v = assemble(base + j, c)
            vh, vm, vl = split3(v)
            th, tm, _ = split3(v.T)
            g_s[...] += bdot(jnp.concatenate([th, tm], axis=1), jnp.concatenate([vh, vm], axis=0))
            a_s[...] += bdot(jnp.concatenate([th, th], axis=1), jnp.concatenate([vm, vl], axis=0))
            apply_v(j, 1)

        loop(0, n, gram)

        a = a_s[...]
        g = g_s[...] + (a + a.T)
        na = 4 * (ia % 2) + ia // 2
        nb = 4 * (ib % 2) + ib // 2
        diag = []
        t_rows = pl.ds(pl.multiple_of(32 * (8 - n), 32), 32)
        for xx in (0, 1):
            for cc in (0, 1):
                raw = tbuf[cc, xx, t_rows, :]
                e = jnp.where(c == cc, raw, pltpu.roll(raw, 64, 1))
                diag += [e, e]
        t4 = jnp.concatenate(diag, axis=0)
        t = jnp.where(ia == ib, jnp.concatenate([t4, t4], axis=1), 0.0)
        for lev in (1, 2, 4):
            pick = (na // (2 * lev) == nb // (2 * lev)) & ((na // lev) % 2 == 0) & ((nb // lev) % 2 == 1)
            t = t - fdot(fdot(t, jnp.where(pick, g, 0.0)), t)
        tx[n - 1, c] = t.T
        t_copy(n, c).start()

        def solve(h):
            yh, ym, yl = split3(fdot(w_s[...], tx[n - 1, h]))
            return jnp.concatenate([yh, ym, yl], axis=0)

        def update(j, y3):
            rows = pl.ds(pl.multiple_of(j * 512, 512), 512)
            d1 = ndot(y3, vh_s[rows, :])
            d2 = ndot(y3[:256], vm_s[rows, :])
            d3 = ndot(y3[:128], vl_s[rows, :])
            xt[8 - n + j] -= (((d3 + d1[256:]) + d2[128:]) + (d2[:128] + d1[128:256])) + d1[:128]

        t_copy(n, 1 - c).wait_recv()
        y_s[...] = solve(1)
        w_s[...] = jnp.zeros_like(w_s)

        def middle(j):
            @pl.when(n < 8)
            def _():
                share(n, n + j)

            update(j, y_s[...])
            apply_v(j, 0)

        loop(0, n, middle)
        y_s[...] = solve(0)

        def last(j):
            @pl.when(n < 8)
            def _():
                share(n, 2 * n + j)

            update(j, y_s[...])

        loop(0, n, last)


    loop(1, 9, pair)

    def turn_out(u):
        stage[u] = xt[u].T.reshape(2, 4, 64, 128)

        def z_out(r):
            pltpu.make_async_copy(stage.at[u, lax.rem(r, 2), place(r)], o_ref.at[r, u], in_sem.at[1]).start()

        loop(0, 8, z_out)

    loop(0, 8, turn_out)

    remote(buf.at[c, x, y, 0:3], z_sem.at[0], x_dev, 0).wait_send()
    remote(buf.at[c, x, y], x1_sem.at[0], x_dev, 1).wait_send()
    remote(buf.at[c, x, y], y1_sem.at[0], y_dev, 2).wait_send()
    remote(buf.at[c, 1 - x, y, 0], y2_sem.at[0], y_dev, 3).wait_send()
    remote(buf.at[c, x, 1 - y, 0], x2_sem.at[0], x_dev, 4).wait_send()
    remote(buf.at[c, 1 - x, 1 - y, 0:2], z2_sem.at[0], z2_dev, 9).wait_send()
    remote(buf.at[c], p_sem.at[0], p_dev, 5).wait_send()
    t_x.wait_send()
    t_p[0].wait_send()
    t_p[1].wait_send()
    remote(tx.at[:, 0], tx_sem.at[0], p_dev, 10).wait_send()
    pltpu.make_async_copy(stage, stage, in_sem.at[1]).wait()


def solution(mesh):
    def local_apply(v_loc, t_loc, z_loc):
        out = pl.pallas_call(
            fused_kernel,
            out_shape=jax.ShapeDtypeStruct((8, 8, 64, 128), F32),
            in_specs=[pl.BlockSpec(memory_space=pl.ANY)] * 3,
            out_specs=pl.BlockSpec(memory_space=pl.ANY),
            scratch_shapes=[
                pltpu.VMEM((2, 2, 2, 4, 64 * UNITS, 128), F32),
                pltpu.VMEM((32, 32, 32), F32),
                pltpu.VMEM((2, 2, 256, 128), F32),
                pltpu.VMEM((8, 2, 4, 64, 128), F32),
                pltpu.VMEM((8, 128, 512), F32),
                pltpu.VMEM((8, 2, 256, 256), F32),
                pltpu.VMEM((4096, 256), BF16),
                pltpu.VMEM((4096, 256), BF16),
                pltpu.VMEM((4096, 256), BF16),
                pltpu.VMEM((256, 256), F32),
                pltpu.VMEM((256, 256), F32),
                pltpu.VMEM((128, 256), F32),
                pltpu.VMEM((384, 256), BF16),
                pltpu.SemaphoreType.DMA((3,)),
                pltpu.SemaphoreType.DMA((11,)),
                pltpu.SemaphoreType.DMA((UNITS,)),
                pltpu.SemaphoreType.DMA((UNITS,)),
                pltpu.SemaphoreType.DMA((UNITS,)),
                pltpu.SemaphoreType.DMA((UNITS,)),
                pltpu.SemaphoreType.DMA((UNITS,)),
                pltpu.SemaphoreType.DMA((UNITS,)),
                pltpu.SemaphoreType.DMA((UNITS,)),
                pltpu.SemaphoreType.DMA((3,)),
                pltpu.SemaphoreType.DMA((8,)),
            ],
            compiler_params=pltpu.CompilerParams(
                collective_id=0, has_side_effects=True, vmem_limit_bytes=66 * 1000 * 1000
            ),
            name="gather_apply",
        )(v_loc, t_loc, z_loc.reshape(8, 8, 64, 128))
        return out.reshape(4096, 128)

    return jax.shard_map(
        local_apply,
        mesh=mesh,
        in_specs=(P("row", "col"), P("col", None, None), P(None, ("row", "col"))),
        out_specs=P(None, ("row", "col")),
        check_vma=False,
    )
```

```python
import functools
import jax
import jax.numpy as jnp
from jax import lax
from jax.experimental import pallas as pl
from jax.experimental.pallas import tpu as pltpu
from jax.sharding import PartitionSpec as P

F32 = jnp.float32
BF16 = jnp.bfloat16
HI = lax.Precision.HIGHEST
MESH = pl.DeviceIdType.MESH
UNITS = 36
Z_AHEAD = 4
EARLY = 6
D1 = 3
D2 = 2
D3 = 3
LAG = D1 + D2 + D3


def split3(v):
    h = v.astype(BF16)
    r = v - h.astype(F32)
    m = r.astype(BF16)
    l = (r - m.astype(F32)).astype(BF16)
    return h, m, l


def bdot(a, b):
    return jnp.dot(a, b, preferred_element_type=F32)


def ndot(a, b):
    return lax.dot_general(a, b, (((1,), (1,)), ((), ())), preferred_element_type=F32)


def fdot(a, b):
    return jnp.dot(a, b, precision=HI, preferred_element_type=F32)


def loop(lo, hi, body):
    def step(i, carry):
        body(i)
        return carry

    lax.fori_loop(lo, hi, step, 0)


def fused_kernel(
    v_ref, t_ref, z_ref, o_ref, buf, traw, tbuf, stage, xt, tx, vh_s, vm_s, vl_s, g_s, a_s, w_s, y_s,
    in_sem, send_sem, z_sem, x1_sem, y1_sem, x2_sem, y2_sem, z2_sem, p_sem, t_sem, tx_sem,
):
    row, col = lax.axis_index("row"), lax.axis_index("col")
    z, y = row // 2, lax.rem(row, 2)
    x, c = col // 2, lax.rem(col, 2)
    x_dev = (row, (1 - x) * 2 + c)
    y_dev = (z * 2 + 1 - y, col)
    p_dev = (row, x * 2 + 1 - c)
    low_z = lax.rem(z, 2)
    slot = 2 * low_z + z // 2
    z2_dev = ((z + 1 - 2 * low_z) * 2 + y, col)
    z_devs = [(lax.rem(z + k, 4) * 2 + y, col) for k in (1, 2, 3)]

    def unit(q):
        return pl.ds(pl.multiple_of(64 * q, 64), 64)

    def remote(view, recv, dev, kind):
        return pltpu.make_async_remote_copy(
            src_ref=view, dst_ref=view, send_sem=send_sem.at[kind], recv_sem=recv, device_id=dev, device_id_type=MESH
        )

    def z_copy(q, k):
        return remote(buf.at[c, x, y, slot, unit(q)], z_sem.at[q], z_devs[k], 0)

    def x1_copy(q):
        return remote(buf.at[c, x, y, :, unit(q)], x1_sem.at[q], x_dev, 1)

    def y1_copy(q):
        return remote(buf.at[c, x, y, :, unit(q)], y1_sem.at[q], y_dev, 2)

    def xy_piece(q, k):
        view = buf.at[c, x, y, lax.rem(slot + k, 4), unit(q)]
        return remote(view, x1_sem.at[q], x_dev, 1), remote(view, y1_sem.at[q], y_dev, 2)

    def y2_copy(q):
        return remote(buf.at[c, 1 - x, y, 2 * low_z, unit(q)], y2_sem.at[q], y_dev, 3)

    def x2_copy(q):
        return remote(buf.at[c, x, 1 - y, 2 * low_z + 1, unit(q)], x2_sem.at[q], x_dev, 4)

    def z2_copy(q):
        return remote(buf.at[c, 1 - x, 1 - y, pl.ds(2 * low_z, 2), unit(q)], z2_sem.at[q], z2_dev, 9)

    def p_copy(q, xx, yy):
        return remote(buf.at[c, xx, yy, :, unit(q)], p_sem.at[q], p_dev, 5)

    def z_land(q):
        return remote(buf.at[c, x, y, 0:3, unit(q)], z_sem.at[q], x_dev, 0)

    def x1_land(q):
        return remote(buf.at[c, 1 - x, y, :, unit(q)], x1_sem.at[q], x_dev, 1)

    def y1_land(q):
        return remote(buf.at[c, x, 1 - y, :, unit(q)], y1_sem.at[q], y_dev, 2)

    def y2_land(q):
        return remote(buf.at[c, 1 - x, 1 - y, 2 * low_z, unit(q)], y2_sem.at[q], y_dev, 3)

    def x2_land(q):
        return remote(buf.at[c, 1 - x, 1 - y, 2 * low_z + 1, unit(q)], x2_sem.at[q], x_dev, 4)

    def z2_land(q):
        return remote(buf.at[c, 1 - x, 1 - y, pl.ds(2 - 2 * low_z, 2), unit(q)], z2_sem.at[q], z2_dev, 9)

    def p_land(q):
        return remote(buf.at[1 - c, :, :, :, unit(q)], p_sem.at[q], p_dev, 5)

    def z_send(q):
        for k in range(3):
            z_copy(q, k).start()

    def comm(q):
        @pl.when(q + Z_AHEAD < UNITS)
        def _():
            z_send(q + Z_AHEAD)

        q1 = q - D1

        @pl.when((q1 >= 0) & (q1 < UNITS))
        def _():
            x1_land(q1).wait_recv()
            y2_copy(q1).start()
            y1_land(q1).wait_recv()
            x2_copy(q1).start()
            p_copy(q1, 1 - x, y).start()
            p_copy(q1, x, 1 - y).start()

        @pl.when(q < UNITS)
        def _():
            z_land(q).wait_recv()

            @pl.when(q < EARLY)
            def _():
                for k in (1, 2, 3):
                    for copy in xy_piece(q, k):
                        copy.start()

            @pl.when(q >= EARLY)
            def _():
                x1_copy(q).start()
                y1_copy(q).start()

            p_copy(q, x, y).start()

        q2 = q - D1 - D2

        @pl.when((q2 >= 0) & (q2 < UNITS))
        def _():
            y2_land(q2).wait_recv()
            x2_land(q2).wait_recv()
            z2_copy(q2).start()

        q3 = q - LAG

        @pl.when((q3 >= 0) & (q3 < UNITS))
        def _():
            z2_land(q3).wait_recv()
            p_copy(q3, 1 - x, 1 - y).start()

    def first_unit(n):
        return n * (n - 1) // 2

    def v_in(n, j):
        src = v_ref.at[pl.ds(pl.multiple_of(64 * (8 - n + j), 64), 64), pl.ds(pl.multiple_of(128 * (8 - n), 128), 128)]
        return pltpu.make_async_copy(src, buf.at[c, x, y, slot, unit(first_unit(n) + j)], in_sem.at[0])

    def place(r):
        return 2 * lax.rem(r // 2, 2) + r // 4

    def z_in(r):
        return pltpu.make_async_copy(z_ref.at[r], stage.at[:, lax.rem(r, 2), place(r)], in_sem.at[1])

    t_in = pltpu.make_async_copy(t_ref, traw, in_sem.at[2])
    loop(1, 9, lambda n: loop(0, n, lambda j: v_in(n, j).start()))
    t_in.start()
    loop(0, 8, lambda r: z_in(r).start())

    barrier = pltpu.get_barrier_semaphore()
    for dev in [x_dev, y_dev, p_dev] + z_devs:
        pl.semaphore_signal(barrier, inc=1, device_id=dev, device_id_type=MESH)
    own = buf.at[c, x, y, slot]
    pltpu.make_async_copy(own, own, in_sem.at[0]).wait()
    pl.semaphore_wait(barrier, 6)

    loop(0, Z_AHEAD, z_send)

    def early(q):
        for copy in xy_piece(q, 0):
            copy.start()

    loop(0, EARLY, early)
    t_in.wait()

    def pack_t(b):
        rows = pl.ds(pl.multiple_of(32 * b, 32), 32)
        tbuf[c, x, rows, :] = jnp.concatenate([traw[4 * b + k] for k in range(4)], axis=1)

    loop(0, 8, pack_t)
    loop(0, 2, comm)
    t_x = remote(tbuf.at[c, x], t_sem.at[0], x_dev, 6)
    t_p = [remote(tbuf.at[c, x], t_sem.at[1], p_dev, 7), remote(tbuf.at[c, 1 - x], t_sem.at[2], p_dev, 8)]
    t_x.start()
    t_p[0].start()
    loop(2, 1 + LAG, comm)
    remote(tbuf.at[c, 1 - x], t_sem.at[0], x_dev, 6).wait_recv()
    t_p[1].start()
    pltpu.make_async_copy(stage, stage, in_sem.at[1]).wait()

    def turn_in(u):
        xt[u] = stage[u].reshape(512, 128).T

    loop(0, 8, turn_in)
    remote(tbuf.at[1 - c, x], t_sem.at[1], p_dev, 7).wait_recv()
    remote(tbuf.at[1 - c, 1 - x], t_sem.at[2], p_dev, 8).wait_recv()

    ia = lax.broadcasted_iota(jnp.int32, (256, 256), 0) // 32
    ib = lax.broadcasted_iota(jnp.int32, (256, 256), 1) // 32
    low = lax.broadcasted_iota(jnp.int32, (512, 128), 1) // 64

    def steps(n):
        return first_unit(n) + LAG + n - n // 4 - 2 * (n // 8)

    def share(n, at):
        grow = steps(n + 1) - steps(n)
        loop(steps(n) + at * grow // (3 * n), steps(n) + (at + 1) * grow // (3 * n), comm)

    def assemble(q, h):
        cols = []
        for xx in (0, 1):
            same = buf[h, xx, :, :, unit(q), :].reshape(512, 128)
            other = buf[1 - h, xx, :, :, unit(q), :].reshape(512, 128)
            cols.append(jnp.where(low == h, same, pltpu.roll(other, 64, 1)))
        return jnp.concatenate(cols, axis=1)

    def t_copy(n, half):
        return remote(tx.at[n - 1, half], tx_sem.at[n - 1], p_dev, 10)

    def pair(n):
        base = first_unit(n)
        g_s[...] = jnp.zeros_like(g_s)
        a_s[...] = jnp.zeros_like(a_s)
        w_s[...] = jnp.zeros_like(w_s)

        def block(j, k, h):
            return jnp.concatenate([assemble(base + j + i, h) for i in range(k)], axis=0)

        def rows_of(j, k):
            return pl.ds(pl.multiple_of(j * 512, 512), 512 * k)

        def apply_v(j, k, h):
            vh, vm, vl = split3(block(j, k, h))
            rows = rows_of(j, k)
            vh_s[rows, :] = vh
            vm_s[rows, :] = vm
            vl_s[rows, :] = vl
            xh, xm, xl = split3(jnp.concatenate([xt[8 - n + j + i] for i in range(k)], axis=1))
            p1 = bdot(jnp.concatenate([xh, xm, xl], axis=0), vh)
            p2 = bdot(jnp.concatenate([xh, xm], axis=0), vm)
            p3 = bdot(xh, vl)
            w_s[...] += (((p3 + p1[256:]) + p2[128:]) + (p2[:128] + p1[128:256])) + p1[:128]

        def gram(j, k):
            for i in range(k):
                @pl.when(n < 8)
                def _():
                    share(n, j + i)

                @pl.when(n == 8)
                def _():
                    grow = UNITS + LAG - steps(8)
                    loop(steps(8) + (j + i) * grow // 8, steps(8) + (j + i + 1) * grow // 8, comm)

            for i in range(k):
                p_land(base + j + i).wait_recv()
            v = block(j, k, c)
            vh, vm, vl = split3(v)
            th, tm, _ = split3(v.T)
            g_s[...] += bdot(jnp.concatenate([th, tm], axis=1), jnp.concatenate([vh, vm], axis=0))
            a_s[...] += bdot(jnp.concatenate([th, th], axis=1), jnp.concatenate([vm, vl], axis=0))
            apply_v(j, k, 1)

        def twos(body):
            loop(0, n // 2, lambda i: body(2 * i, 2))

            @pl.when(lax.rem(n, 2) == 1)
            def _():
                body(n - 1, 1)

        twos(gram)

        a = a_s[...]
        g = g_s[...] + (a + a.T)
        na = 4 * (ia % 2) + ia // 2
        nb = 4 * (ib % 2) + ib // 2
        diag = []
        t_rows = pl.ds(pl.multiple_of(32 * (8 - n), 32), 32)
        for xx in (0, 1):
            for cc in (0, 1):
                raw = tbuf[cc, xx, t_rows, :]
                e = jnp.where(c == cc, raw, pltpu.roll(raw, 64, 1))
                diag += [e, e]
        t4 = jnp.concatenate(diag, axis=0)
        t = jnp.where(ia == ib, jnp.concatenate([t4, t4], axis=1), 0.0)
        for lev in (1, 2, 4):
            pick = (na // (2 * lev) == nb // (2 * lev)) & ((na // lev) % 2 == 0) & ((nb // lev) % 2 == 1)
            t = t - fdot(fdot(t, jnp.where(pick, g, 0.0)), t)
        tx[n - 1, c] = t.T
        t_copy(n, c).start()

        def solve(h):
            yh, ym, yl = split3(fdot(w_s[...], tx[n - 1, h]))
            return jnp.concatenate([yh, ym, yl], axis=0)

        def update(j, k, y3):
            rows = rows_of(j, k)
            d1 = ndot(y3, vh_s[rows, :])
            d2 = ndot(y3[:256], vm_s[rows, :])
            d3 = ndot(y3[:128], vl_s[rows, :])
            d = (((d3 + d1[256:]) + d2[128:]) + (d2[:128] + d1[128:256])) + d1[:128]
            for i in range(k):
                xt[8 - n + j + i] -= d[:, 512 * i : 512 * i + 512]

        t_copy(n, 1 - c).wait_recv()
        y_s[...] = solve(1)
        w_s[...] = jnp.zeros_like(w_s)

        def middle(j, k):
            for i in range(k):
                @pl.when(n < 8)
                def _():
                    share(n, n + j + i)

            update(j, k, y_s[...])
            apply_v(j, k, 0)

        twos(middle)
        y_s[...] = solve(0)

        def last(j, k):
            for i in range(k):
                @pl.when(n < 8)
                def _():
                    share(n, 2 * n + j + i)

            update(j, k, y_s[...])

        twos(last)


    loop(1, 9, pair)

    def turn_out(u):
        stage[u] = xt[u].T.reshape(2, 4, 64, 128)

        def z_out(r):
            pltpu.make_async_copy(stage.at[u, lax.rem(r, 2), place(r)], o_ref.at[r, u], in_sem.at[1]).start()

        loop(0, 8, z_out)

    loop(0, 8, turn_out)

    remote(buf.at[c, x, y, 0:3], z_sem.at[0], x_dev, 0).wait_send()
    remote(buf.at[c, x, y], x1_sem.at[0], x_dev, 1).wait_send()
    remote(buf.at[c, x, y], y1_sem.at[0], y_dev, 2).wait_send()
    remote(buf.at[c, 1 - x, y, 0], y2_sem.at[0], y_dev, 3).wait_send()
    remote(buf.at[c, x, 1 - y, 0], x2_sem.at[0], x_dev, 4).wait_send()
    remote(buf.at[c, 1 - x, 1 - y, 0:2], z2_sem.at[0], z2_dev, 9).wait_send()
    remote(buf.at[c], p_sem.at[0], p_dev, 5).wait_send()
    t_x.wait_send()
    t_p[0].wait_send()
    t_p[1].wait_send()
    remote(tx.at[:, 0], tx_sem.at[0], p_dev, 10).wait_send()
    pltpu.make_async_copy(stage, stage, in_sem.at[1]).wait()


def solution(mesh):
    def local_apply(v_loc, t_loc, z_loc):
        out = pl.pallas_call(
            fused_kernel,
            out_shape=jax.ShapeDtypeStruct((8, 8, 64, 128), F32),
            in_specs=[pl.BlockSpec(memory_space=pl.ANY)] * 3,
            out_specs=pl.BlockSpec(memory_space=pl.ANY),
            scratch_shapes=[
                pltpu.VMEM((2, 2, 2, 4, 64 * UNITS, 128), F32),
                pltpu.VMEM((32, 32, 32), F32),
                pltpu.VMEM((2, 2, 256, 128), F32),
                pltpu.VMEM((8, 2, 4, 64, 128), F32),
                pltpu.VMEM((8, 128, 512), F32),
                pltpu.VMEM((8, 2, 256, 256), F32),
                pltpu.VMEM((4096, 256), BF16),
                pltpu.VMEM((4096, 256), BF16),
                pltpu.VMEM((4096, 256), BF16),
                pltpu.VMEM((256, 256), F32),
                pltpu.VMEM((256, 256), F32),
                pltpu.VMEM((128, 256), F32),
                pltpu.VMEM((384, 256), BF16),
                pltpu.SemaphoreType.DMA((3,)),
                pltpu.SemaphoreType.DMA((11,)),
                pltpu.SemaphoreType.DMA((UNITS,)),
                pltpu.SemaphoreType.DMA((UNITS,)),
                pltpu.SemaphoreType.DMA((UNITS,)),
                pltpu.SemaphoreType.DMA((UNITS,)),
                pltpu.SemaphoreType.DMA((UNITS,)),
                pltpu.SemaphoreType.DMA((UNITS,)),
                pltpu.SemaphoreType.DMA((UNITS,)),
                pltpu.SemaphoreType.DMA((3,)),
                pltpu.SemaphoreType.DMA((8,)),
            ],
            compiler_params=pltpu.CompilerParams(
                collective_id=0, has_side_effects=True, vmem_limit_bytes=66 * 1000 * 1000
            ),
            name="gather_apply",
        )(v_loc, t_loc, z_loc.reshape(8, 8, 64, 128))
        return out.reshape(4096, 128)

    return jax.shard_map(
        local_apply,
        mesh=mesh,
        in_specs=(P("row", "col"), P("col", None, None), P(None, ("row", "col"))),
        out_specs=P(None, ("row", "col")),
        check_vma=False,
    )
```

```python
import functools
import jax
import jax.numpy as jnp
from jax import lax
from jax.experimental import pallas as pl
from jax.experimental.pallas import tpu as pltpu
from jax.sharding import PartitionSpec as P

F32 = jnp.float32
BF16 = jnp.bfloat16
HI = lax.Precision.HIGHEST
MESH = pl.DeviceIdType.MESH
UNITS = 36
Z_AHEAD = 3
GRAM, MERGE, MIDDLE, LAST = 9, 46, 8, 4
EARLY = 6
D1 = 3
D2 = 2
D3 = 3
LAG = D1 + D2 + D3


def split3(v):
    h = v.astype(BF16)
    r = v - h.astype(F32)
    m = r.astype(BF16)
    l = (r - m.astype(F32)).astype(BF16)
    return h, m, l


def bdot(a, b):
    return jnp.dot(a, b, preferred_element_type=F32)


def ndot(a, b):
    return lax.dot_general(a, b, (((1,), (1,)), ((), ())), preferred_element_type=F32)


def fdot(a, b):
    return jnp.dot(a, b, precision=HI, preferred_element_type=F32)


def loop(lo, hi, body):
    def step(i, carry):
        body(i)
        return carry

    lax.fori_loop(lo, hi, step, 0)


def fused_kernel(
    v_ref, t_ref, z_ref, o_ref, buf, traw, tbuf, stage, xt, tx, vh_s, vm_s, vl_s, g_s, a_s, w_s, y_s, t_s,
    in_sem, send_sem, z_sem, x1_sem, y1_sem, x2_sem, y2_sem, z2_sem, p_sem, t_sem, tx_sem,
):
    row, col = lax.axis_index("row"), lax.axis_index("col")
    z, y = row // 2, lax.rem(row, 2)
    x, c = col // 2, lax.rem(col, 2)
    x_dev = (row, (1 - x) * 2 + c)
    y_dev = (z * 2 + 1 - y, col)
    p_dev = (row, x * 2 + 1 - c)
    low_z = lax.rem(z, 2)
    slot = 2 * low_z + z // 2
    z2_dev = ((z + 1 - 2 * low_z) * 2 + y, col)
    z_devs = [(lax.rem(z + k, 4) * 2 + y, col) for k in (1, 2, 3)]

    def unit(q):
        return pl.ds(pl.multiple_of(64 * q, 64), 64)

    def remote(view, recv, dev, kind):
        return pltpu.make_async_remote_copy(
            src_ref=view, dst_ref=view, send_sem=send_sem.at[kind], recv_sem=recv, device_id=dev, device_id_type=MESH
        )

    def z_copy(q, k):
        return remote(buf.at[c, x, y, slot, unit(q)], z_sem.at[q], z_devs[k], 0)

    def x1_copy(q):
        return remote(buf.at[c, x, y, :, unit(q)], x1_sem.at[q], x_dev, 1)

    def y1_copy(q):
        return remote(buf.at[c, x, y, :, unit(q)], y1_sem.at[q], y_dev, 2)

    def xy_piece(q, k):
        view = buf.at[c, x, y, lax.rem(slot + k, 4), unit(q)]
        return remote(view, x1_sem.at[q], x_dev, 1), remote(view, y1_sem.at[q], y_dev, 2)

    def y2_copy(q):
        return remote(buf.at[c, 1 - x, y, 2 * low_z, unit(q)], y2_sem.at[q], y_dev, 3)

    def x2_copy(q):
        return remote(buf.at[c, x, 1 - y, 2 * low_z + 1, unit(q)], x2_sem.at[q], x_dev, 4)

    def z2_copy(q):
        return remote(buf.at[c, 1 - x, 1 - y, pl.ds(2 * low_z, 2), unit(q)], z2_sem.at[q], z2_dev, 9)

    def p_copy(q, xx, yy):
        return remote(buf.at[c, xx, yy, :, unit(q)], p_sem.at[q], p_dev, 5)

    def z_land(q):
        return remote(buf.at[c, x, y, 0:3, unit(q)], z_sem.at[q], x_dev, 0)

    def x1_land(q):
        return remote(buf.at[c, 1 - x, y, :, unit(q)], x1_sem.at[q], x_dev, 1)

    def y1_land(q):
        return remote(buf.at[c, x, 1 - y, :, unit(q)], y1_sem.at[q], y_dev, 2)

    def y2_land(q):
        return remote(buf.at[c, 1 - x, 1 - y, 2 * low_z, unit(q)], y2_sem.at[q], y_dev, 3)

    def x2_land(q):
        return remote(buf.at[c, 1 - x, 1 - y, 2 * low_z + 1, unit(q)], x2_sem.at[q], x_dev, 4)

    def z2_land(q):
        return remote(buf.at[c, 1 - x, 1 - y, pl.ds(2 - 2 * low_z, 2), unit(q)], z2_sem.at[q], z2_dev, 9)

    def p_land(q):
        return remote(buf.at[1 - c, :, :, :, unit(q)], p_sem.at[q], p_dev, 5)

    def z_send(q):
        for k in range(3):
            z_copy(q, k).start()

    def comm(q):
        @pl.when(q + Z_AHEAD < UNITS)
        def _():
            z_send(q + Z_AHEAD)

        q1 = q - D1

        @pl.when((q1 >= 0) & (q1 < UNITS))
        def _():
            x1_land(q1).wait_recv()
            y2_copy(q1).start()
            y1_land(q1).wait_recv()
            x2_copy(q1).start()
            p_copy(q1, 1 - x, y).start()
            p_copy(q1, x, 1 - y).start()

        @pl.when(q < UNITS)
        def _():
            z_land(q).wait_recv()

            @pl.when(q < EARLY)
            def _():
                for k in (1, 2, 3):
                    for copy in xy_piece(q, k):
                        copy.start()

            @pl.when(q >= EARLY)
            def _():
                x1_copy(q).start()
                y1_copy(q).start()

            p_copy(q, x, y).start()

        q2 = q - D1 - D2

        @pl.when((q2 >= 0) & (q2 < UNITS))
        def _():
            y2_land(q2).wait_recv()
            x2_land(q2).wait_recv()
            z2_copy(q2).start()

        q3 = q - LAG

        @pl.when((q3 >= 0) & (q3 < UNITS))
        def _():
            z2_land(q3).wait_recv()
            p_copy(q3, 1 - x, 1 - y).start()

    def first_unit(n):
        return n * (n - 1) // 2

    def v_in(n, j):
        src = v_ref.at[pl.ds(pl.multiple_of(64 * (8 - n + j), 64), 64), pl.ds(pl.multiple_of(128 * (8 - n), 128), 128)]
        return pltpu.make_async_copy(src, buf.at[c, x, y, slot, unit(first_unit(n) + j)], in_sem.at[0])

    def place(r):
        return 2 * lax.rem(r // 2, 2) + r // 4

    def z_in(r):
        return pltpu.make_async_copy(z_ref.at[r], stage.at[:, lax.rem(r, 2), place(r)], in_sem.at[1])

    t_in = pltpu.make_async_copy(t_ref, traw, in_sem.at[2])
    loop(1, 9, lambda n: loop(0, n, lambda j: v_in(n, j).start()))
    t_in.start()
    loop(0, 8, lambda r: z_in(r).start())

    barrier = pltpu.get_barrier_semaphore()
    for dev in [x_dev, y_dev, p_dev] + z_devs:
        pl.semaphore_signal(barrier, inc=1, device_id=dev, device_id_type=MESH)
    own = buf.at[c, x, y, slot]
    pltpu.make_async_copy(own, own, in_sem.at[0]).wait()
    pl.semaphore_wait(barrier, 6)

    loop(0, Z_AHEAD, z_send)

    def early(q):
        for copy in xy_piece(q, 0):
            copy.start()

    loop(0, EARLY, early)
    t_in.wait()

    def pack_t(b):
        rows = pl.ds(pl.multiple_of(32 * b, 32), 32)
        tbuf[c, x, rows, :] = jnp.concatenate([traw[4 * b + k] for k in range(4)], axis=1)

    loop(0, 8, pack_t)
    loop(0, 2, comm)
    t_x = remote(tbuf.at[c, x], t_sem.at[0], x_dev, 6)
    t_p = [remote(tbuf.at[c, x], t_sem.at[1], p_dev, 7), remote(tbuf.at[c, 1 - x], t_sem.at[2], p_dev, 8)]
    t_x.start()
    t_p[0].start()
    loop(2, 1 + LAG, comm)
    remote(tbuf.at[c, 1 - x], t_sem.at[0], x_dev, 6).wait_recv()
    t_p[1].start()
    pltpu.make_async_copy(stage, stage, in_sem.at[1]).wait()

    def turn_in(u):
        xt[u] = stage[u].reshape(512, 128).T

    loop(0, 8, turn_in)
    remote(tbuf.at[1 - c, x], t_sem.at[1], p_dev, 7).wait_recv()
    remote(tbuf.at[1 - c, 1 - x], t_sem.at[2], p_dev, 8).wait_recv()

    ia = lax.broadcasted_iota(jnp.int32, (256, 256), 0) // 32
    ib = lax.broadcasted_iota(jnp.int32, (256, 256), 1) // 32
    low = lax.broadcasted_iota(jnp.int32, (512, 128), 1) // 64

    def steps(n):
        return first_unit(n) + LAG + n - n // 4 - 2 * (n // 8)

    def share(n, start, end):
        grow, whole = steps(n + 1) - steps(n), (GRAM + MIDDLE + LAST) * n + MERGE

        @pl.when(n < 8)
        def _():
            loop(steps(n) + start * grow // whole, steps(n) + end * grow // whole, comm)

    def assemble(q, h):
        cols = []
        for xx in (0, 1):
            same = buf[h, xx, :, :, unit(q), :].reshape(512, 128)
            other = buf[1 - h, xx, :, :, unit(q), :].reshape(512, 128)
            cols.append(jnp.where(low == h, same, pltpu.roll(other, 64, 1)))
        return jnp.concatenate(cols, axis=1)

    def t_copy(n, half):
        return remote(tx.at[n - 1, half], tx_sem.at[n - 1], p_dev, 10)

    def pair(n):
        base = first_unit(n)
        g_s[...] = jnp.zeros_like(g_s)
        a_s[...] = jnp.zeros_like(a_s)
        w_s[...] = jnp.zeros_like(w_s)

        def block(j, k, h):
            return jnp.concatenate([assemble(base + j + i, h) for i in range(k)], axis=0)

        def rows_of(j, k):
            return pl.ds(pl.multiple_of(j * 512, 512), 512 * k)

        def apply_v(j, k, h):
            vh, vm, vl = split3(block(j, k, h))
            rows = rows_of(j, k)
            vh_s[rows, :] = vh
            vm_s[rows, :] = vm
            vl_s[rows, :] = vl
            xh, xm, xl = split3(jnp.concatenate([xt[8 - n + j + i] for i in range(k)], axis=1))
            p1 = bdot(jnp.concatenate([xh, xm, xl], axis=0), vh)
            p2 = bdot(jnp.concatenate([xh, xm], axis=0), vm)
            p3 = bdot(xh, vl)
            w_s[...] += (((p3 + p1[256:]) + p2[128:]) + (p2[:128] + p1[128:256])) + p1[:128]

        def gram(j, k):
            for i in range(k):
                share(n, GRAM * (j + i), GRAM * (j + i + 1))

                @pl.when(n == 8)
                def _():
                    grow = UNITS + LAG - steps(8)
                    loop(steps(8) + (j + i) * grow // 8, steps(8) + (j + i + 1) * grow // 8, comm)

            for i in range(k):
                p_land(base + j + i).wait_recv()
            v = block(j, k, c)
            vh, vm, vl = split3(v)
            th, tm, _ = split3(v.T)
            g_s[...] += bdot(jnp.concatenate([th, tm], axis=1), jnp.concatenate([vh, vm], axis=0))
            a_s[...] += bdot(jnp.concatenate([th, th], axis=1), jnp.concatenate([vm, vl], axis=0))
            apply_v(j, k, 1)

        def twos(body):
            loop(0, n // 2, lambda i: body(2 * i, 2))

            @pl.when(lax.rem(n, 2) == 1)
            def _():
                body(n - 1, 1)

        twos(gram)

        a = a_s[...]
        g = g_s[...] + (a + a.T)
        diag = []
        t_rows = pl.ds(pl.multiple_of(32 * (8 - n), 32), 32)
        for xx in (0, 1):
            for cc in (0, 1):
                raw = tbuf[cc, xx, t_rows, :]
                e = jnp.where(c == cc, raw, pltpu.roll(raw, 64, 1))
                diag += [e, e]
        t4 = jnp.concatenate(diag, axis=0)
        one = ia[:128, :128], ib[:128, :128]
        first = (one[0] % 2 == one[1] % 2) & (one[0] // 2 == 0) & (one[1] // 2 == 1)
        merged = []
        for k in (0, 128):
            d = jnp.where(one[0] == one[1], t4[k : k + 128], 0.0)
            merged.append(d - fdot(fdot(d, jnp.where(first, g[k : k + 128, k : k + 128], 0.0)), d))
        cross = fdot(fdot(merged[0], jnp.where(one[0] % 2 == one[1] % 2, g[:128, 128:], 0.0)), merged[1])
        t_s[:128, :128] = merged[0]
        t_s[:128, 128:] = -cross
        t_s[128:, :128] = jnp.zeros((128, 128), F32)
        t_s[128:, 128:] = merged[1]
        g_s[...] = jnp.where((ia % 2 == 0) & (ib % 2 == 1), g, 0.0)
        share(n, GRAM * n, GRAM * n + MERGE // 2)
        t = t_s[...]
        t = t - fdot(fdot(t, g_s[...]), t)
        tx[n - 1, c] = t.T
        t_copy(n, c).start()
        share(n, GRAM * n + MERGE // 2, GRAM * n + MERGE)

        def solve(h):
            yh, ym, yl = split3(fdot(w_s[...], tx[n - 1, h]))
            return jnp.concatenate([yh, ym, yl], axis=0)

        def update(j, k, y3):
            rows = rows_of(j, k)
            d1 = ndot(y3, vh_s[rows, :])
            d2 = ndot(y3[:256], vm_s[rows, :])
            d3 = ndot(y3[:128], vl_s[rows, :])
            d = (((d3 + d1[256:]) + d2[128:]) + (d2[:128] + d1[128:256])) + d1[:128]
            for i in range(k):
                xt[8 - n + j + i] -= d[:, 512 * i : 512 * i + 512]

        t_copy(n, 1 - c).wait_recv()
        y_s[...] = solve(1)
        w_s[...] = jnp.zeros_like(w_s)

        def middle(j, k):
            start = GRAM * n + MERGE + MIDDLE * j
            share(n, start, start + MIDDLE * k)
            update(j, k, y_s[...])
            apply_v(j, k, 0)

        twos(middle)
        y_s[...] = solve(0)

        def last(j, k):
            start = (GRAM + MIDDLE) * n + MERGE + LAST * j
            share(n, start, start + LAST * k)
            update(j, k, y_s[...])

        twos(last)


    loop(1, 9, pair)

    def turn_out(u):
        stage[u] = xt[u].T.reshape(2, 4, 64, 128)

        def z_out(r):
            pltpu.make_async_copy(stage.at[u, lax.rem(r, 2), place(r)], o_ref.at[r, u], in_sem.at[1]).start()

        loop(0, 8, z_out)

    loop(0, 8, turn_out)

    remote(buf.at[c, x, y, 0:3], z_sem.at[0], x_dev, 0).wait_send()
    remote(buf.at[c, x, y], x1_sem.at[0], x_dev, 1).wait_send()
    remote(buf.at[c, x, y], y1_sem.at[0], y_dev, 2).wait_send()
    remote(buf.at[c, 1 - x, y, 0], y2_sem.at[0], y_dev, 3).wait_send()
    remote(buf.at[c, x, 1 - y, 0], x2_sem.at[0], x_dev, 4).wait_send()
    remote(buf.at[c, 1 - x, 1 - y, 0:2], z2_sem.at[0], z2_dev, 9).wait_send()
    remote(buf.at[c], p_sem.at[0], p_dev, 5).wait_send()
    t_x.wait_send()
    t_p[0].wait_send()
    t_p[1].wait_send()
    remote(tx.at[:, 0], tx_sem.at[0], p_dev, 10).wait_send()
    pltpu.make_async_copy(stage, stage, in_sem.at[1]).wait()


def solution(mesh):
    def local_apply(v_loc, t_loc, z_loc):
        out = pl.pallas_call(
            fused_kernel,
            out_shape=jax.ShapeDtypeStruct((8, 8, 64, 128), F32),
            in_specs=[pl.BlockSpec(memory_space=pl.ANY)] * 3,
            out_specs=pl.BlockSpec(memory_space=pl.ANY),
            scratch_shapes=[
                pltpu.VMEM((2, 2, 2, 4, 64 * UNITS, 128), F32),
                pltpu.VMEM((32, 32, 32), F32),
                pltpu.VMEM((2, 2, 256, 128), F32),
                pltpu.VMEM((8, 2, 4, 64, 128), F32),
                pltpu.VMEM((8, 128, 512), F32),
                pltpu.VMEM((8, 2, 256, 256), F32),
                pltpu.VMEM((4096, 256), BF16),
                pltpu.VMEM((4096, 256), BF16),
                pltpu.VMEM((4096, 256), BF16),
                pltpu.VMEM((256, 256), F32),
                pltpu.VMEM((256, 256), F32),
                pltpu.VMEM((128, 256), F32),
                pltpu.VMEM((384, 256), BF16),
                pltpu.VMEM((256, 256), F32),
                pltpu.SemaphoreType.DMA((3,)),
                pltpu.SemaphoreType.DMA((11,)),
                pltpu.SemaphoreType.DMA((UNITS,)),
                pltpu.SemaphoreType.DMA((UNITS,)),
                pltpu.SemaphoreType.DMA((UNITS,)),
                pltpu.SemaphoreType.DMA((UNITS,)),
                pltpu.SemaphoreType.DMA((UNITS,)),
                pltpu.SemaphoreType.DMA((UNITS,)),
                pltpu.SemaphoreType.DMA((UNITS,)),
                pltpu.SemaphoreType.DMA((3,)),
                pltpu.SemaphoreType.DMA((8,)),
            ],
            compiler_params=pltpu.CompilerParams(
                collective_id=0, has_side_effects=True, vmem_limit_bytes=66 * 1000 * 1000
            ),
            name="gather_apply",
        )(v_loc, t_loc, z_loc.reshape(8, 8, 64, 128))
        return out.reshape(4096, 128)

    return jax.shard_map(
        local_apply,
        mesh=mesh,
        in_specs=(P("row", "col"), P("col", None, None), P(None, ("row", "col"))),
        out_specs=P(None, ("row", "col")),
        check_vma=False,
    )
```

```python
import functools
import jax
import jax.numpy as jnp
from jax import lax
from jax.experimental import pallas as pl
from jax.experimental.pallas import tpu as pltpu
from jax.sharding import PartitionSpec as P

F32 = jnp.float32
BF16 = jnp.bfloat16
HI = lax.Precision.HIGHEST
MESH = pl.DeviceIdType.MESH
UNITS = 36
Z_AHEAD = 3
GRAM, MERGE, MIDDLE, LAST = 9, 46, 8, 4
EARLY = 6
D1 = 2
D2 = 2
D3 = 2
LAG = D1 + D2 + D3


def split3(v):
    h = v.astype(BF16)
    r = v - h.astype(F32)
    m = r.astype(BF16)
    l = (r - m.astype(F32)).astype(BF16)
    return h, m, l


def bdot(a, b):
    return jnp.dot(a, b, preferred_element_type=F32)


def ndot(a, b):
    return lax.dot_general(a, b, (((1,), (1,)), ((), ())), preferred_element_type=F32)


def fdot(a, b):
    return jnp.dot(a, b, precision=HI, preferred_element_type=F32)


def loop(lo, hi, body):
    def step(i, carry):
        body(i)
        return carry

    lax.fori_loop(lo, hi, step, 0)


def fused_kernel(
    v_ref, t_ref, z_ref, o_ref, buf, traw, tbuf, stage, xt, tx, vh_s, vm_s, vl_s, g_s, a_s, w_s, y_s, t_s,
    in_sem, send_sem, z_sem, x1_sem, y1_sem, x2_sem, y2_sem, z2_sem, p_sem, t_sem, tx_sem,
):
    row, col = lax.axis_index("row"), lax.axis_index("col")
    z, y = row // 2, lax.rem(row, 2)
    x, c = col // 2, lax.rem(col, 2)
    x_dev = (row, (1 - x) * 2 + c)
    y_dev = (z * 2 + 1 - y, col)
    p_dev = (row, x * 2 + 1 - c)
    low_z = lax.rem(z, 2)
    slot = 2 * low_z + z // 2
    z2_dev = ((z + 1 - 2 * low_z) * 2 + y, col)
    z_devs = [(lax.rem(z + k, 4) * 2 + y, col) for k in (1, 2, 3)]

    def unit(q):
        return pl.ds(pl.multiple_of(64 * q, 64), 64)

    def remote(view, recv, dev, kind):
        return pltpu.make_async_remote_copy(
            src_ref=view, dst_ref=view, send_sem=send_sem.at[kind], recv_sem=recv, device_id=dev, device_id_type=MESH
        )

    def z_copy(q, k):
        return remote(buf.at[c, x, y, slot, unit(q)], z_sem.at[q], z_devs[k], 0)

    def x1_copy(q):
        return remote(buf.at[c, x, y, :, unit(q)], x1_sem.at[q], x_dev, 1)

    def y1_copy(q):
        return remote(buf.at[c, x, y, :, unit(q)], y1_sem.at[q], y_dev, 2)

    def xy_piece(q, k):
        view = buf.at[c, x, y, lax.rem(slot + k, 4), unit(q)]
        return remote(view, x1_sem.at[q], x_dev, 1), remote(view, y1_sem.at[q], y_dev, 2)

    def y2_copy(q):
        return remote(buf.at[c, 1 - x, y, 2 * low_z, unit(q)], y2_sem.at[q], y_dev, 3)

    def x2_copy(q):
        return remote(buf.at[c, x, 1 - y, 2 * low_z + 1, unit(q)], x2_sem.at[q], x_dev, 4)

    def z2_copy(q):
        return remote(buf.at[c, 1 - x, 1 - y, pl.ds(2 * low_z, 2), unit(q)], z2_sem.at[q], z2_dev, 9)

    def p_copy(q, xx, yy):
        return remote(buf.at[c, xx, yy, :, unit(q)], p_sem.at[q], p_dev, 5)

    def z_land(q):
        return remote(buf.at[c, x, y, 0:3, unit(q)], z_sem.at[q], x_dev, 0)

    def x1_land(q):
        return remote(buf.at[c, 1 - x, y, :, unit(q)], x1_sem.at[q], x_dev, 1)

    def y1_land(q):
        return remote(buf.at[c, x, 1 - y, :, unit(q)], y1_sem.at[q], y_dev, 2)

    def y2_land(q):
        return remote(buf.at[c, 1 - x, 1 - y, 2 * low_z, unit(q)], y2_sem.at[q], y_dev, 3)

    def x2_land(q):
        return remote(buf.at[c, 1 - x, 1 - y, 2 * low_z + 1, unit(q)], x2_sem.at[q], x_dev, 4)

    def z2_land(q):
        return remote(buf.at[c, 1 - x, 1 - y, pl.ds(2 - 2 * low_z, 2), unit(q)], z2_sem.at[q], z2_dev, 9)

    def p_land(q):
        return remote(buf.at[1 - c, :, :, :, unit(q)], p_sem.at[q], p_dev, 5)

    def z_send(q):
        for k in range(3):
            z_copy(q, k).start()

    def comm(q):
        @pl.when(q + Z_AHEAD < UNITS)
        def _():
            z_send(q + Z_AHEAD)

        q1 = q - D1

        @pl.when((q1 >= 0) & (q1 < UNITS))
        def _():
            x1_land(q1).wait_recv()
            y2_copy(q1).start()
            y1_land(q1).wait_recv()
            x2_copy(q1).start()
            p_copy(q1, 1 - x, y).start()
            p_copy(q1, x, 1 - y).start()

        @pl.when(q < UNITS)
        def _():
            z_land(q).wait_recv()

            @pl.when(q < EARLY)
            def _():
                for k in (1, 2, 3):
                    for copy in xy_piece(q, k):
                        copy.start()

            @pl.when(q >= EARLY)
            def _():
                x1_copy(q).start()
                y1_copy(q).start()

            p_copy(q, x, y).start()

        q2 = q - D1 - D2

        @pl.when((q2 >= 0) & (q2 < UNITS))
        def _():
            y2_land(q2).wait_recv()
            x2_land(q2).wait_recv()
            z2_copy(q2).start()

        q3 = q - LAG

        @pl.when((q3 >= 0) & (q3 < UNITS))
        def _():
            z2_land(q3).wait_recv()
            p_copy(q3, 1 - x, 1 - y).start()

    def first_unit(n):
        return n * (n - 1) // 2

    def v_in(n, j):
        src = v_ref.at[pl.ds(pl.multiple_of(64 * (8 - n + j), 64), 64), pl.ds(pl.multiple_of(128 * (8 - n), 128), 128)]
        return pltpu.make_async_copy(src, buf.at[c, x, y, slot, unit(first_unit(n) + j)], in_sem.at[0])

    def place(r):
        return 2 * lax.rem(r // 2, 2) + r // 4

    def z_in(r):
        return pltpu.make_async_copy(z_ref.at[r], stage.at[:, lax.rem(r, 2), place(r)], in_sem.at[1])

    t_in = pltpu.make_async_copy(t_ref, traw, in_sem.at[2])
    loop(1, 9, lambda n: loop(0, n, lambda j: v_in(n, j).start()))
    t_in.start()
    loop(0, 8, lambda r: z_in(r).start())

    barrier = pltpu.get_barrier_semaphore()
    for dev in [x_dev, y_dev, p_dev] + z_devs:
        pl.semaphore_signal(barrier, inc=1, device_id=dev, device_id_type=MESH)
    own = buf.at[c, x, y, slot]
    pltpu.make_async_copy(own, own, in_sem.at[0]).wait()
    pl.semaphore_wait(barrier, 6)

    loop(0, Z_AHEAD, z_send)

    def early(q):
        for copy in xy_piece(q, 0):
            copy.start()

    loop(0, EARLY, early)
    t_in.wait()

    def pack_t(b):
        rows = pl.ds(pl.multiple_of(32 * b, 32), 32)
        tbuf[c, x, rows, :] = jnp.concatenate([traw[4 * b + k] for k in range(4)], axis=1)

    loop(0, 8, pack_t)
    loop(0, 2, comm)
    t_x = remote(tbuf.at[c, x], t_sem.at[0], x_dev, 6)
    t_p = [remote(tbuf.at[c, x], t_sem.at[1], p_dev, 7), remote(tbuf.at[c, 1 - x], t_sem.at[2], p_dev, 8)]
    t_x.start()
    t_p[0].start()
    loop(2, 1 + LAG, comm)
    remote(tbuf.at[c, 1 - x], t_sem.at[0], x_dev, 6).wait_recv()
    t_p[1].start()
    pltpu.make_async_copy(stage, stage, in_sem.at[1]).wait()

    def turn_in(u):
        xt[u] = stage[u].reshape(512, 128).T

    loop(0, 8, turn_in)
    remote(tbuf.at[1 - c, x], t_sem.at[1], p_dev, 7).wait_recv()
    remote(tbuf.at[1 - c, 1 - x], t_sem.at[2], p_dev, 8).wait_recv()

    ia = lax.broadcasted_iota(jnp.int32, (256, 256), 0) // 32
    ib = lax.broadcasted_iota(jnp.int32, (256, 256), 1) // 32
    low = lax.broadcasted_iota(jnp.int32, (512, 128), 1) // 64

    def steps(n):
        return first_unit(n) + LAG + n - n // 4 - 2 * (n // 8)

    def share(n, start, end):
        grow, whole = steps(n + 1) - steps(n), (GRAM + MIDDLE + LAST) * n + MERGE

        @pl.when(n < 8)
        def _():
            loop(steps(n) + start * grow // whole, steps(n) + end * grow // whole, comm)

    def assemble(q, h):
        cols = []
        for xx in (0, 1):
            same = buf[h, xx, :, :, unit(q), :].reshape(512, 128)
            other = buf[1 - h, xx, :, :, unit(q), :].reshape(512, 128)
            cols.append(jnp.where(low == h, same, pltpu.roll(other, 64, 1)))
        return jnp.concatenate(cols, axis=1)

    def t_copy(n, half):
        return remote(tx.at[n - 1, half], tx_sem.at[n - 1], p_dev, 10)

    def pair(n):
        base = first_unit(n)
        g_s[...] = jnp.zeros_like(g_s)
        a_s[...] = jnp.zeros_like(a_s)
        w_s[...] = jnp.zeros_like(w_s)

        def block(j, k, h):
            return jnp.concatenate([assemble(base + j + i, h) for i in range(k)], axis=0)

        def rows_of(j, k):
            return pl.ds(pl.multiple_of(j * 512, 512), 512 * k)

        def apply_v(j, k, h):
            vh, vm, vl = split3(block(j, k, h))
            rows = rows_of(j, k)
            vh_s[rows, :] = vh
            vm_s[rows, :] = vm
            vl_s[rows, :] = vl
            xh, xm, xl = split3(jnp.concatenate([xt[8 - n + j + i] for i in range(k)], axis=1))
            p1 = bdot(jnp.concatenate([xh, xm, xl], axis=0), vh)
            p2 = bdot(jnp.concatenate([xh, xm], axis=0), vm)
            p3 = bdot(xh, vl)
            w_s[...] += (((p3 + p1[256:]) + p2[128:]) + (p2[:128] + p1[128:256])) + p1[:128]

        def gram(j, k):
            for i in range(k):
                share(n, GRAM * (j + i), GRAM * (j + i + 1))

                @pl.when(n == 8)
                def _():
                    grow = UNITS + LAG - steps(8)
                    loop(steps(8) + (j + i) * grow // 8, steps(8) + (j + i + 1) * grow // 8, comm)

            for i in range(k):
                p_land(base + j + i).wait_recv()
            v = block(j, k, c)
            vh, vm, vl = split3(v)
            th, tm, _ = split3(v.T)
            g_s[...] += bdot(jnp.concatenate([th, tm], axis=1), jnp.concatenate([vh, vm], axis=0))
            a_s[...] += bdot(jnp.concatenate([th, th], axis=1), jnp.concatenate([vm, vl], axis=0))
            apply_v(j, k, 1)

        def twos(body):
            loop(0, n // 2, lambda i: body(2 * i, 2))

            @pl.when(lax.rem(n, 2) == 1)
            def _():
                body(n - 1, 1)

        twos(gram)

        a = a_s[...]
        g = g_s[...] + (a + a.T)
        diag = []
        t_rows = pl.ds(pl.multiple_of(32 * (8 - n), 32), 32)
        for xx in (0, 1):
            for cc in (0, 1):
                raw = tbuf[cc, xx, t_rows, :]
                e = jnp.where(c == cc, raw, pltpu.roll(raw, 64, 1))
                diag += [e, e]
        t4 = jnp.concatenate(diag, axis=0)
        one = ia[:128, :128], ib[:128, :128]
        first = (one[0] % 2 == one[1] % 2) & (one[0] // 2 == 0) & (one[1] // 2 == 1)
        merged = []
        for k in (0, 128):
            d = jnp.where(one[0] == one[1], t4[k : k + 128], 0.0)
            merged.append(d - fdot(fdot(d, jnp.where(first, g[k : k + 128, k : k + 128], 0.0)), d))
        cross = fdot(fdot(merged[0], jnp.where(one[0] % 2 == one[1] % 2, g[:128, 128:], 0.0)), merged[1])
        t_s[:128, :128] = merged[0]
        t_s[:128, 128:] = -cross
        t_s[128:, :128] = jnp.zeros((128, 128), F32)
        t_s[128:, 128:] = merged[1]
        g_s[...] = jnp.where((ia % 2 == 0) & (ib % 2 == 1), g, 0.0)
        share(n, GRAM * n, GRAM * n + MERGE // 2)
        t = t_s[...]
        t = t - fdot(fdot(t, g_s[...]), t)
        tx[n - 1, c] = t.T
        t_copy(n, c).start()
        share(n, GRAM * n + MERGE // 2, GRAM * n + MERGE)

        def solve(h):
            yh, ym, yl = split3(fdot(w_s[...], tx[n - 1, h]))
            return jnp.concatenate([yh, ym, yl], axis=0)

        def update(j, k, y3):
            rows = rows_of(j, k)
            d1 = ndot(y3, vh_s[rows, :])
            d2 = ndot(y3[:256], vm_s[rows, :])
            d3 = ndot(y3[:128], vl_s[rows, :])
            d = (((d3 + d1[256:]) + d2[128:]) + (d2[:128] + d1[128:256])) + d1[:128]
            for i in range(k):
                xt[8 - n + j + i] -= d[:, 512 * i : 512 * i + 512]

        t_copy(n, 1 - c).wait_recv()
        y_s[...] = solve(1)
        w_s[...] = jnp.zeros_like(w_s)

        def middle(j, k):
            start = GRAM * n + MERGE + MIDDLE * j
            share(n, start, start + MIDDLE * k)
            update(j, k, y_s[...])
            apply_v(j, k, 0)

        twos(middle)
        y_s[...] = solve(0)

        def last(j, k):
            start = (GRAM + MIDDLE) * n + MERGE + LAST * j
            share(n, start, start + LAST * k)
            update(j, k, y_s[...])

        twos(last)


    loop(1, 9, pair)

    def turn_out(u):
        stage[u] = xt[u].T.reshape(2, 4, 64, 128)

        def z_out(r):
            pltpu.make_async_copy(stage.at[u, lax.rem(r, 2), place(r)], o_ref.at[r, u], in_sem.at[1]).start()

        loop(0, 8, z_out)

    loop(0, 8, turn_out)

    remote(buf.at[c, x, y, 0:3], z_sem.at[0], x_dev, 0).wait_send()
    remote(buf.at[c, x, y], x1_sem.at[0], x_dev, 1).wait_send()
    remote(buf.at[c, x, y], y1_sem.at[0], y_dev, 2).wait_send()
    remote(buf.at[c, 1 - x, y, 0], y2_sem.at[0], y_dev, 3).wait_send()
    remote(buf.at[c, x, 1 - y, 0], x2_sem.at[0], x_dev, 4).wait_send()
    remote(buf.at[c, 1 - x, 1 - y, 0:2], z2_sem.at[0], z2_dev, 9).wait_send()
    remote(buf.at[c], p_sem.at[0], p_dev, 5).wait_send()
    t_x.wait_send()
    t_p[0].wait_send()
    t_p[1].wait_send()
    remote(tx.at[:, 0], tx_sem.at[0], p_dev, 10).wait_send()
    pltpu.make_async_copy(stage, stage, in_sem.at[1]).wait()


def solution(mesh):
    def local_apply(v_loc, t_loc, z_loc):
        out = pl.pallas_call(
            fused_kernel,
            out_shape=jax.ShapeDtypeStruct((8, 8, 64, 128), F32),
            in_specs=[pl.BlockSpec(memory_space=pl.ANY)] * 3,
            out_specs=pl.BlockSpec(memory_space=pl.ANY),
            scratch_shapes=[
                pltpu.VMEM((2, 2, 2, 4, 64 * UNITS, 128), F32),
                pltpu.VMEM((32, 32, 32), F32),
                pltpu.VMEM((2, 2, 256, 128), F32),
                pltpu.VMEM((8, 2, 4, 64, 128), F32),
                pltpu.VMEM((8, 128, 512), F32),
                pltpu.VMEM((8, 2, 256, 256), F32),
                pltpu.VMEM((4096, 256), BF16),
                pltpu.VMEM((4096, 256), BF16),
                pltpu.VMEM((4096, 256), BF16),
                pltpu.VMEM((256, 256), F32),
                pltpu.VMEM((256, 256), F32),
                pltpu.VMEM((128, 256), F32),
                pltpu.VMEM((384, 256), BF16),
                pltpu.VMEM((256, 256), F32),
                pltpu.SemaphoreType.DMA((3,)),
                pltpu.SemaphoreType.DMA((11,)),
                pltpu.SemaphoreType.DMA((UNITS,)),
                pltpu.SemaphoreType.DMA((UNITS,)),
                pltpu.SemaphoreType.DMA((UNITS,)),
                pltpu.SemaphoreType.DMA((UNITS,)),
                pltpu.SemaphoreType.DMA((UNITS,)),
                pltpu.SemaphoreType.DMA((UNITS,)),
                pltpu.SemaphoreType.DMA((UNITS,)),
                pltpu.SemaphoreType.DMA((3,)),
                pltpu.SemaphoreType.DMA((8,)),
            ],
            compiler_params=pltpu.CompilerParams(
                collective_id=0, has_side_effects=True, vmem_limit_bytes=66 * 1000 * 1000
            ),
            name="gather_apply",
        )(v_loc, t_loc, z_loc.reshape(8, 8, 64, 128))
        return out.reshape(4096, 128)

    return jax.shard_map(
        local_apply,
        mesh=mesh,
        in_specs=(P("row", "col"), P("col", None, None), P(None, ("row", "col"))),
        out_specs=P(None, ("row", "col")),
        check_vma=False,
    )
```

```python
import functools
import jax
import jax.numpy as jnp
from jax import lax
from jax.experimental import pallas as pl
from jax.experimental.pallas import tpu as pltpu
from jax.sharding import PartitionSpec as P

F32 = jnp.float32
BF16 = jnp.bfloat16
HI = lax.Precision.HIGHEST
MESH = pl.DeviceIdType.MESH
UNITS = 36
Z_AHEAD = 3
GRAM, MERGE, MIDDLE, LAST = 9, 46, 8, 4
EARLY = 6
D1 = 2
D2 = 2
D3 = 2
LAG = D1 + D2 + D3


def split3(v):
    h = v.astype(BF16)
    r = v - h.astype(F32)
    m = r.astype(BF16)
    l = (r - m.astype(F32)).astype(BF16)
    return h, m, l


def bdot(a, b):
    return jnp.dot(a, b, preferred_element_type=F32)


def ndot(a, b):
    return lax.dot_general(a, b, (((1,), (1,)), ((), ())), preferred_element_type=F32)


def fdot(a, b):
    return jnp.dot(a, b, precision=HI, preferred_element_type=F32)


def loop(lo, hi, body):
    def step(i, carry):
        body(i)
        return carry

    lax.fori_loop(lo, hi, step, 0)


def fused_kernel(
    v_ref, t_ref, z_ref, o_ref, buf, traw, tbuf, stage, xt, tx, vh_s, vm_s, vl_s, g_s, a_s, w_s, y_s, t_s,
    in_sem, send_sem, z_sem, x1_sem, y1_sem, x2_sem, y2_sem, z2_sem, p_sem, t_sem, tx_sem,
):
    row, col = lax.axis_index("row"), lax.axis_index("col")
    z, y = row // 2, lax.rem(row, 2)
    x, c = col // 2, lax.rem(col, 2)
    x_dev = (row, (1 - x) * 2 + c)
    y_dev = (z * 2 + 1 - y, col)
    p_dev = (row, x * 2 + 1 - c)
    low_z = lax.rem(z, 2)
    slot = 2 * low_z + z // 2
    z2_dev = ((z + 1 - 2 * low_z) * 2 + y, col)
    z_devs = [(lax.rem(z + k, 4) * 2 + y, col) for k in (1, 2, 3)]

    def unit(q):
        return pl.ds(pl.multiple_of(64 * q, 64), 64)

    def remote(view, recv, dev, kind):
        return pltpu.make_async_remote_copy(
            src_ref=view, dst_ref=view, send_sem=send_sem.at[kind], recv_sem=recv, device_id=dev, device_id_type=MESH
        )

    def z_copy(q, k):
        return remote(buf.at[c, x, y, slot, unit(q)], z_sem.at[q], z_devs[k], 0)

    def x1_copy(q):
        return remote(buf.at[c, x, y, :, unit(q)], x1_sem.at[q], x_dev, 1)

    def y1_copy(q):
        return remote(buf.at[c, x, y, :, unit(q)], y1_sem.at[q], y_dev, 2)

    def xy_piece(q, k):
        view = buf.at[c, x, y, lax.rem(slot + k, 4), unit(q)]
        return remote(view, x1_sem.at[q], x_dev, 1), remote(view, y1_sem.at[q], y_dev, 2)

    def y2_copy(q):
        return remote(buf.at[c, 1 - x, y, 2 * low_z, unit(q)], y2_sem.at[q], y_dev, 3)

    def x2_copy(q):
        return remote(buf.at[c, x, 1 - y, 2 * low_z + 1, unit(q)], x2_sem.at[q], x_dev, 4)

    def z2_copy(q):
        return remote(buf.at[c, 1 - x, 1 - y, pl.ds(2 * low_z, 2), unit(q)], z2_sem.at[q], z2_dev, 9)

    def p_copy(q, xx, yy):
        return remote(buf.at[c, xx, yy, :, unit(q)], p_sem.at[q], p_dev, 5)

    def z_land(q):
        return remote(buf.at[c, x, y, 0:3, unit(q)], z_sem.at[q], x_dev, 0)

    def x1_land(q):
        return remote(buf.at[c, 1 - x, y, :, unit(q)], x1_sem.at[q], x_dev, 1)

    def y1_land(q):
        return remote(buf.at[c, x, 1 - y, :, unit(q)], y1_sem.at[q], y_dev, 2)

    def y2_land(q):
        return remote(buf.at[c, 1 - x, 1 - y, 2 * low_z, unit(q)], y2_sem.at[q], y_dev, 3)

    def x2_land(q):
        return remote(buf.at[c, 1 - x, 1 - y, 2 * low_z + 1, unit(q)], x2_sem.at[q], x_dev, 4)

    def z2_land(q):
        return remote(buf.at[c, 1 - x, 1 - y, pl.ds(2 - 2 * low_z, 2), unit(q)], z2_sem.at[q], z2_dev, 9)

    def p_land(q):
        return remote(buf.at[1 - c, :, :, :, unit(q)], p_sem.at[q], p_dev, 5)

    def z_send(q):
        for k in range(3):
            z_copy(q, k).start()

    def comm(q):
        @pl.when(q + Z_AHEAD < UNITS)
        def _():
            z_send(q + Z_AHEAD)

        q1 = q - D1

        @pl.when((q1 >= 0) & (q1 < UNITS))
        def _():
            x1_land(q1).wait_recv()
            y2_copy(q1).start()
            y1_land(q1).wait_recv()
            x2_copy(q1).start()
            p_copy(q1, 1 - x, y).start()
            p_copy(q1, x, 1 - y).start()

        @pl.when(q < UNITS)
        def _():
            z_land(q).wait_recv()

            @pl.when(q < EARLY)
            def _():
                for k in (1, 2, 3):
                    for copy in xy_piece(q, k):
                        copy.start()

            @pl.when(q >= EARLY)
            def _():
                x1_copy(q).start()
                y1_copy(q).start()

            p_copy(q, x, y).start()

        q2 = q - D1 - D2

        @pl.when((q2 >= 0) & (q2 < UNITS))
        def _():
            y2_land(q2).wait_recv()
            x2_land(q2).wait_recv()
            z2_copy(q2).start()

        q3 = q - LAG

        @pl.when((q3 >= 0) & (q3 < UNITS))
        def _():
            z2_land(q3).wait_recv()
            p_copy(q3, 1 - x, 1 - y).start()

    def first_unit(n):
        return n * (n - 1) // 2

    def v_in(n, j):
        src = v_ref.at[pl.ds(pl.multiple_of(64 * (8 - n + j), 64), 64), pl.ds(pl.multiple_of(128 * (8 - n), 128), 128)]
        return pltpu.make_async_copy(src, buf.at[c, x, y, slot, unit(first_unit(n) + j)], in_sem.at[0])

    def place(r):
        return 2 * lax.rem(r // 2, 2) + r // 4

    def z_in(r):
        return pltpu.make_async_copy(z_ref.at[r], stage.at[:, lax.rem(r, 2), place(r)], in_sem.at[1])

    t_in = pltpu.make_async_copy(t_ref, traw, in_sem.at[2])
    loop(1, 9, lambda n: loop(0, n, lambda j: v_in(n, j).start()))
    t_in.start()
    loop(0, 8, lambda r: z_in(r).start())

    barrier = pltpu.get_barrier_semaphore()
    for dev in [x_dev, y_dev, p_dev] + z_devs:
        pl.semaphore_signal(barrier, inc=1, device_id=dev, device_id_type=MESH)
    own = buf.at[c, x, y, slot]
    pltpu.make_async_copy(own, own, in_sem.at[0]).wait()
    pl.semaphore_wait(barrier, 6)

    loop(0, Z_AHEAD, z_send)

    def early(q):
        for copy in xy_piece(q, 0):
            copy.start()

    loop(0, EARLY, early)
    t_in.wait()

    def pack_t(b):
        rows = pl.ds(pl.multiple_of(32 * b, 32), 32)
        tbuf[c, x, rows, :] = jnp.concatenate([traw[4 * b + k] for k in range(4)], axis=1)

    loop(0, 8, pack_t)
    loop(0, 2, comm)
    t_x = remote(tbuf.at[c, x], t_sem.at[0], x_dev, 6)
    t_p = [remote(tbuf.at[c, x], t_sem.at[1], p_dev, 7), remote(tbuf.at[c, 1 - x], t_sem.at[2], p_dev, 8)]
    t_x.start()
    t_p[0].start()
    loop(2, 1 + LAG, comm)
    remote(tbuf.at[c, 1 - x], t_sem.at[0], x_dev, 6).wait_recv()
    t_p[1].start()
    pltpu.make_async_copy(stage, stage, in_sem.at[1]).wait()

    def turn_in(u):
        xt[u] = stage[u].reshape(512, 128).T

    loop(0, 8, turn_in)
    remote(tbuf.at[1 - c, x], t_sem.at[1], p_dev, 7).wait_recv()
    remote(tbuf.at[1 - c, 1 - x], t_sem.at[2], p_dev, 8).wait_recv()

    ia = lax.broadcasted_iota(jnp.int32, (256, 256), 0) // 32
    ib = lax.broadcasted_iota(jnp.int32, (256, 256), 1) // 32
    low = lax.broadcasted_iota(jnp.int32, (512, 128), 1) // 64

    def steps(n):
        return first_unit(n) + LAG + n - n // 4 - 2 * (n // 8)

    def share(n, start, end):
        grow, whole = steps(n + 1) - steps(n), (GRAM + MIDDLE + LAST) * n + MERGE

        @pl.when(n < 8)
        def _():
            loop(steps(n) + start * grow // whole, steps(n) + end * grow // whole, comm)

    def assemble(q, h):
        cols = []
        for xx in (0, 1):
            same = buf[h, xx, :, :, unit(q), :].reshape(512, 128)
            other = buf[1 - h, xx, :, :, unit(q), :].reshape(512, 128)
            cols.append(jnp.where(low == h, same, pltpu.roll(other, 64, 1)))
        return jnp.concatenate(cols, axis=1)

    def t_copy(n, half):
        return remote(tx.at[n - 1, half], tx_sem.at[n - 1], p_dev, 10)

    def pair(n):
        base = first_unit(n)
        g_s[...] = jnp.zeros_like(g_s)
        a_s[...] = jnp.zeros_like(a_s)
        w_s[...] = jnp.zeros_like(w_s)

        def block(j, k, h):
            return jnp.concatenate([assemble(base + j + i, h) for i in range(k)], axis=0)

        def rows_of(j, k):
            return pl.ds(pl.multiple_of(j * 512, 512), 512 * k)

        def apply_v(j, k, h):
            vh, vm, vl = split3(block(j, k, h))
            rows = rows_of(j, k)
            vh_s[rows, :] = vh
            vm_s[rows, :] = vm
            vl_s[rows, :] = vl
            xh, xm, xl = split3(jnp.concatenate([xt[8 - n + j + i] for i in range(k)], axis=1))
            p1 = bdot(jnp.concatenate([xh, xm, xl], axis=0), vh)
            p2 = bdot(jnp.concatenate([xh, xm], axis=0), vm)
            p3 = bdot(xh, vl)
            w_s[...] += (((p3 + p1[256:]) + p2[128:]) + (p2[:128] + p1[128:256])) + p1[:128]

        def gram(j, k):
            for i in range(k):
                share(n, GRAM * (j + i), GRAM * (j + i + 1))

                @pl.when(n == 8)
                def _():
                    grow = UNITS + LAG - steps(8)
                    loop(steps(8) + (j + i) * grow // 8, steps(8) + (j + i + 1) * grow // 8, comm)

            for i in range(k):
                p_land(base + j + i).wait_recv()
            v = block(j, k, c)
            vh, vm, vl = split3(v)
            th, tm, _ = split3(v.T)
            g_s[...] += bdot(jnp.concatenate([th, tm], axis=1), jnp.concatenate([vh, vm], axis=0))
            a_s[...] += bdot(jnp.concatenate([th, th], axis=1), jnp.concatenate([vm, vl], axis=0))
            apply_v(j, k, 1)

        def twos(body):
            loop(0, n // 2, lambda i: body(2 * i, 2))

            @pl.when(lax.rem(n, 2) == 1)
            def _():
                body(n - 1, 1)

        twos(gram)

        a = a_s[...]
        g = g_s[...] + (a + a.T)
        diag = []
        t_rows = pl.ds(pl.multiple_of(32 * (8 - n), 32), 32)
        for xx in (0, 1):
            for cc in (0, 1):
                raw = tbuf[cc, xx, t_rows, :]
                e = jnp.where(c == cc, raw, pltpu.roll(raw, 64, 1))
                diag += [e, e]
        t4 = jnp.concatenate(diag, axis=0)
        one = ia[:128, :128], ib[:128, :128]
        first = (one[0] % 2 == one[1] % 2) & (one[0] // 2 == 0) & (one[1] // 2 == 1)
        merged = []
        for k in (0, 128):
            d = jnp.where(one[0] == one[1], t4[k : k + 128], 0.0)
            merged.append(d - fdot(fdot(d, jnp.where(first, g[k : k + 128, k : k + 128], 0.0)), d))
        cross = fdot(fdot(merged[0], jnp.where(one[0] % 2 == one[1] % 2, g[:128, 128:], 0.0)), merged[1])
        t_s[:128, :128] = merged[0]
        t_s[:128, 128:] = -cross
        t_s[128:, :128] = jnp.zeros((128, 128), F32)
        t_s[128:, 128:] = merged[1]
        g_s[...] = jnp.where((ia % 2 == 0) & (ib % 2 == 1), g, 0.0)
        share(n, GRAM * n, GRAM * n + MERGE // 2)
        t = t_s[...]
        t = t - fdot(fdot(t, g_s[...]), t)
        tx[n - 1, c] = t.T
        t_copy(n, c).start()
        share(n, GRAM * n + MERGE // 2, GRAM * n + MERGE)

        def solve(h):
            yh, ym, yl = split3(fdot(w_s[...], tx[n - 1, h]))
            return jnp.concatenate([yh, ym, yl], axis=0)

        def update(j, k, y3):
            rows = rows_of(j, k)
            d1 = ndot(y3, vh_s[rows, :])
            d2 = ndot(y3[:256], vm_s[rows, :])
            d3 = ndot(y3[:128], vl_s[rows, :])
            d = (((d3 + d1[256:]) + d2[128:]) + (d2[:128] + d1[128:256])) + d1[:128]
            for i in range(k):
                xt[8 - n + j + i] -= d[:, 512 * i : 512 * i + 512]

        t_copy(n, 1 - c).wait_recv()
        y_s[...] = solve(1)
        w_s[...] = jnp.zeros_like(w_s)

        def middle(j, k):
            start = GRAM * n + MERGE + MIDDLE * j
            share(n, start, start + MIDDLE * k)
            update(j, k, y_s[...])
            apply_v(j, k, 0)

        twos(middle)
        y_s[...] = solve(0)

        def last(j, k):
            start = (GRAM + MIDDLE) * n + MERGE + LAST * j
            share(n, start, start + LAST * k)
            update(j, k, y_s[...])

        twos(last)


    loop(1, 9, pair)

    def x_out(u):
        return pltpu.make_async_copy(xt.at[u], o_ref.at[u], in_sem.at[1])

    loop(0, 8, lambda u: x_out(u).start())

    remote(buf.at[c, x, y, 0:3], z_sem.at[0], x_dev, 0).wait_send()
    remote(buf.at[c, x, y], x1_sem.at[0], x_dev, 1).wait_send()
    remote(buf.at[c, x, y], y1_sem.at[0], y_dev, 2).wait_send()
    remote(buf.at[c, 1 - x, y, 0], y2_sem.at[0], y_dev, 3).wait_send()
    remote(buf.at[c, x, 1 - y, 0], x2_sem.at[0], x_dev, 4).wait_send()
    remote(buf.at[c, 1 - x, 1 - y, 0:2], z2_sem.at[0], z2_dev, 9).wait_send()
    remote(buf.at[c], p_sem.at[0], p_dev, 5).wait_send()
    t_x.wait_send()
    t_p[0].wait_send()
    t_p[1].wait_send()
    remote(tx.at[:, 0], tx_sem.at[0], p_dev, 10).wait_send()
    pltpu.make_async_copy(xt, xt, in_sem.at[1]).wait()


def turn_kernel(x_ref, o_ref):
    for u in range(2):
        rows = x_ref[u].T
        for r in range(8):
            at = 64 * (4 * (r % 2) + 2 * (r // 2 % 2) + r // 4)
            o_ref[r, u] = rows[at : at + 64]


def solution(mesh):
    def local_apply(v_loc, t_loc, z_loc):
        out = pl.pallas_call(
            fused_kernel,
            out_shape=jax.ShapeDtypeStruct((8, 128, 512), F32),
            in_specs=[pl.BlockSpec(memory_space=pl.ANY)] * 3,
            out_specs=pl.BlockSpec(memory_space=pl.ANY),
            scratch_shapes=[
                pltpu.VMEM((2, 2, 2, 4, 64 * UNITS, 128), F32),
                pltpu.VMEM((32, 32, 32), F32),
                pltpu.VMEM((2, 2, 256, 128), F32),
                pltpu.VMEM((8, 2, 4, 64, 128), F32),
                pltpu.VMEM((8, 128, 512), F32),
                pltpu.VMEM((8, 2, 256, 256), F32),
                pltpu.VMEM((4096, 256), BF16),
                pltpu.VMEM((4096, 256), BF16),
                pltpu.VMEM((4096, 256), BF16),
                pltpu.VMEM((256, 256), F32),
                pltpu.VMEM((256, 256), F32),
                pltpu.VMEM((128, 256), F32),
                pltpu.VMEM((384, 256), BF16),
                pltpu.VMEM((256, 256), F32),
                pltpu.SemaphoreType.DMA((3,)),
                pltpu.SemaphoreType.DMA((11,)),
                pltpu.SemaphoreType.DMA((UNITS,)),
                pltpu.SemaphoreType.DMA((UNITS,)),
                pltpu.SemaphoreType.DMA((UNITS,)),
                pltpu.SemaphoreType.DMA((UNITS,)),
                pltpu.SemaphoreType.DMA((UNITS,)),
                pltpu.SemaphoreType.DMA((UNITS,)),
                pltpu.SemaphoreType.DMA((UNITS,)),
                pltpu.SemaphoreType.DMA((3,)),
                pltpu.SemaphoreType.DMA((8,)),
            ],
            compiler_params=pltpu.CompilerParams(
                collective_id=0, has_side_effects=True, vmem_limit_bytes=66 * 1000 * 1000
            ),
            name="gather_apply",
        )(v_loc, t_loc, z_loc.reshape(8, 8, 64, 128))
        turned = pl.pallas_call(
            turn_kernel,
            grid=(4,),
            out_shape=jax.ShapeDtypeStruct((8, 8, 64, 128), F32),
            in_specs=[pl.BlockSpec((2, 128, 512), lambda u: (u, 0, 0))],
            out_specs=pl.BlockSpec((8, 2, 64, 128), lambda u: (0, u, 0, 0)),
            name="turn",
        )(out)
        return turned.reshape(4096, 128)

    return jax.shard_map(
        local_apply,
        mesh=mesh,
        in_specs=(P("row", "col"), P("col", None, None), P(None, ("row", "col"))),
        out_specs=P(None, ("row", "col")),
        check_vma=False,
    )
```
